128 devices in a mesh: tok: 8 (over x_lo, z), feat: 16 (over y, x_hi, core).
Axes of the slice: x: 4 (x_hi: 2, x_lo: 2; x = x_hi * 2 + x_lo), y: 4, z: 4, core: 2. Of those that a mesh axis runs over, the one named last changes fastest.
Arguments:
- tokens_in: float32 [4096, 16384], P('tok', 'feat'), may hold values from -6 to 6
- key_weight: float32 [16384, 1024], P('feat'), may hold values from -0.046875 to 0.046875
- value_weight: float32 [16384, 1024], P('feat'), may hold values from -0.046875 to 0.046875
- blocks: float32 [4, 64, 256, 256], P(None, 'feat'), may hold values from -0.25 to 1.25, as said below
- row_order: int32 [4, 128], replicated, may hold values from 0 to 127, each once within a row
- key_grad: float32 [4096, 1024], P('tok', 'feat'), may hold values from -0.3 to 0.3
- value_grad: float32 [4096, 1024], P('tok', 'feat'), may hold values from -0.3 to 0.3
- moment: float32 [4, 64, 256, 256], P(None, 'feat', 'tok'), may hold values from -1.8 to 1.8
- second_moment: float32 [4, 64, 256, 256], P(None, 'feat', 'tok'), may hold values from 0.05 to 1
Outputs:
- key_out: float32 [4096, 1024], P('tok', 'feat')
- value_out: float32 [4096, 1024], P('tok', 'feat')
- new_blocks: float32 [4, 64, 256, 256], P(None, 'feat', 'tok')
- new_moment: float32 [4, 64, 256, 256], P(None, 'feat', 'tok')
- new_second: float32 [4, 64, 256, 256], P(None, 'feat', 'tok')
The draws below stay inside these ranges and needn't reach their ends.
Inputs may be any that keep to these rules, and one draw needn't show every extreme that they name: `blocks`: every block is a dense 2 * 128 x 2 * 128 matrix. Each row of row_order is a permutation.
All inputs are finite; a program needn't handle non-finite values.
Results may differ from the reference program's by a relative error of at most 0.0001.
Values sent between devices are 32-bit elements; how exact they have to be, the bound alone decides.
A program may use at most 128 MiB of HBM per device.

```python
import math
import jax
import jax.numpy as jnp
import numpy as np
from jax import lax

D = 16384
KV = 1024
HALF = 128
FACTORS = 4
TOKENS = 4096
BLOCKS = 64
N_FEAT = 16


def draw_blocks(key, part):
    noise_key, diagonal_key = jax.random.split(jax.random.fold_in(key, 17))
    shape_full = (FACTORS, BLOCKS, 2 * HALF, 2 * HALF)
    noise = jnp.clip(jax.random.normal(noise_key, shape_full, jnp.float32), -4.0, 4.0) * 0.0625
    diagonal_part = jax.random.uniform(diagonal_key, (FACTORS, BLOCKS, 2 * HALF), jnp.float32, 0.6, 1.0)
    return noise + diagonal_part[..., None] * jnp.eye(2 * HALF, dtype=jnp.float32)


def levels(own_key, shape, cuts, least, top_value):
    level = 1.0
    for position, shards_of in cuts:
        heights = jax.random.uniform(jax.random.fold_in(jax.random.fold_in(own_key, 6), position), (shards_of,), jnp.float32, least / len(cuts), top_value / len(cuts))
        level = level * jnp.repeat(jnp.exp(heights), shape[position] // shards_of).reshape((-1,) + (1,) * (len(shape) - 1 - position))
    return level


def gaussian(stream_key, shape, scale, bound, cuts=(), kind=jnp.bfloat16):
    loudness = levels(stream_key, shape, cuts, -0.22, 0.18) if cuts else 1.0
    values = jax.random.normal(stream_key, shape, jnp.float32) * scale * loudness
    return jnp.minimum(jnp.maximum(values, -bound), bound).astype(kind)


def setup_inputs(seed: int = 0) -> dict:
    splits = jax.random.split(jax.random.key(seed), 10)
    tokens_in = gaussian(splits[0], (TOKENS, D), 1.0, 6.0, ((0, 8), (1, 16)), jnp.float32)
    key_weight = gaussian(splits[1], (D, KV), D ** -0.5, 0.046875, ((0, 16),), jnp.float32)
    value_weight = gaussian(splits[2], (D, KV), D ** -0.5, 0.046875, ((0, 16),), jnp.float32)
    blocks = draw_blocks(jax.random.fold_in(splits[9], 71), 0)
    row_order = jax.vmap(lambda own: jax.random.permutation(own, HALF))(jax.random.split(splits[4], FACTORS)).reshape((FACTORS, HALF)).astype(jnp.int32)
    key_grad = gaussian(splits[5], (TOKENS, KV), 0.05, 0.3, ((0, 8), (1, 16)), jnp.float32)
    value_grad = gaussian(splits[6], (TOKENS, KV), 0.05, 0.3, ((0, 8), (1, 16)), jnp.float32)
    moment = gaussian(splits[7], (FACTORS, BLOCKS, 2 * HALF, 2 * HALF), 0.3, 1.8, ((1, 16), (2, 8)), jnp.float32)
    second_moment = jnp.clip(jnp.exp(math.log(1.0) - 2.9957323 * jax.random.uniform(splits[8], (FACTORS, BLOCKS, 2 * HALF, 2 * HALF), jnp.float32) ** levels(splits[8], (FACTORS, BLOCKS, 2 * HALF, 2 * HALF), ((1, 16), (2, 8)), -0.2, 0.2)), 0.05, 1.0)
    return {"tokens_in": tokens_in, "key_weight": key_weight, "value_weight": value_weight, "blocks": blocks, "row_order": row_order, "key_grad": key_grad, "value_grad": value_grad, "moment": moment, "second_moment": second_moment}


highest = lax.Precision.HIGHEST
beta_one = 0.9
beta_two = 0.95
learn_rate = 0.01
epsilon = 1e-08
bias_one = 1.0 - 0.9 ** 10
bias_two = 1.0 - 0.95 ** 10

def pair_tables(factor, halves_dev, feat_count):
    blocks_dev = halves_dev // 2
    bit_list = [0, 1, feat_count.bit_length() - 2]
    first_list = []
    second_list = []
    for block_index in range(blocks_dev * feat_count):
        owner_dev = block_index // blocks_dev
        slot_index = block_index % blocks_dev
        if factor == 0:
            first_half = owner_dev * halves_dev + 2 * slot_index
            second_half = first_half + 1
        else:
            stride = 1 << bit_list[factor - 1]
            if owner_dev // stride % 2 == 0:
                first_half = owner_dev * halves_dev + slot_index
                second_half = (owner_dev + stride) * halves_dev + slot_index
            else:
                first_half = (owner_dev - stride) * halves_dev + blocks_dev + slot_index
                second_half = owner_dev * halves_dev + blocks_dev + slot_index
        first_list.append(first_half)
        second_list.append(second_half)
    return (np.array(first_list, np.int32), np.array(second_list, np.int32))

def apply_factor(rotated, applied, first_index, second_index):
    token_count, width = rotated.shape
    halves = rotated.reshape(token_count, -1, HALF)
    paired = jnp.concatenate([halves[:, first_index], halves[:, second_index]], axis=2)
    turned = jnp.einsum('tbi,bij->tbj', paired, applied, precision=highest)
    result = jnp.zeros_like(halves)
    result = result.at[:, first_index].set(turned[:, :, :HALF])
    result = result.at[:, second_index].set(turned[:, :, HALF:])
    return result.reshape(token_count, width)

def reference(tokens_in, key_weight, value_weight, blocks, row_order, key_grad, value_grad, moment, second_moment):
    halves_dev = D // (HALF * N_FEAT)
    tables = [pair_tables(factor, halves_dev, N_FEAT) for factor in range(FACTORS)]

    def forward(block_values):
        rotated = tokens_in
        for factor in range(FACTORS):
            rows = jnp.concatenate([row_order[factor], row_order[factor] + HALF]).astype(jnp.int32)
            applied = jnp.take(block_values[factor], rows, axis=1)
            rotated = apply_factor(rotated, applied, tables[factor][0], tables[factor][1])
        key_part = jnp.dot(rotated, key_weight, precision=highest, preferred_element_type=jnp.float32)
        value_part = jnp.dot(rotated, value_weight, precision=highest, preferred_element_type=jnp.float32)
        return (key_part, value_part)
    outputs, pullback = jax.vjp(forward, blocks)
    key_out, value_out = outputs
    block_grad = pullback((key_grad, value_grad))[0]
    new_moment = beta_one * moment + (1.0 - beta_one) * block_grad
    new_second = beta_two * second_moment + (1.0 - beta_two) * block_grad * block_grad
    step_size = learn_rate * (new_moment / bias_one) / (jnp.sqrt(new_second / bias_two) + epsilon)
    new_blocks = blocks - step_size
    return (key_out, value_out, new_blocks, new_moment, new_second)
```

```python
import jax
import jax.numpy as jnp
from jax import lax
from jax.experimental import pallas as pl
from jax.experimental.pallas import tpu as pltpu
from jax.sharding import PartitionSpec as P

MESH = pl.DeviceIdType.MESH
F32 = jnp.float32
BF16 = jnp.bfloat16
beta_one = 0.9
beta_two = 0.95
learn_rate = 0.01
epsilon = 1e-08
bias_one = 1.0 - 0.9**10
bias_two = 1.0 - 0.95**10

CT = 128
NC = 4
HT = 256


def split(v):
    hi = v.astype(BF16)
    lo = (v - hi.astype(F32)).astype(BF16)
    return hi, lo


def dims(ca, cb):
    return (((ca,), (cb,)), ((), ()))


def dot3(ah, al, bh, bl, ca=1, cb=0):
    d = dims(ca, cb)
    out = lax.dot_general(ah, bh, d, preferred_element_type=F32)
    out = out + lax.dot_general(ah, bl, d, preferred_element_type=F32)
    return out + lax.dot_general(al, bh, d, preferred_element_type=F32)


def kernel(
    x, kw, vw, bl, ro, kv, mo, se,
    ko, vo, nb, nm, ns,
    XP, WH, WL, AH, AL, TT, TS, ST, BS, R, I, T, G, J, GKV, KT, KP, LH, LL, YL, XL, FT, GO, GL, XG, AD,
    bsem, xsem, stsem, ktsem, adsem, osem,
    ss, rs, kvs, kvr, gs, gr, ps, pr, zs, zr, us, ur,
):
    tok = lax.axis_index("tok")
    feat = lax.axis_index("feat")
    z = lax.rem(tok, 4)
    xlo = lax.div(tok, 4)
    core = lax.rem(feat, 2)
    xhi = lax.rem(lax.div(feat, 2), 2)
    y = lax.div(feat, 4)
    yhi = lax.div(feat, 8)
    yx = lax.rem(feat, 4)
    chip = lax.div(feat, 2)
    bits = [None, core, xhi, yhi]
    steps = [None, 1, 2, 8]

    def flip(m):
        return (tok, feat + steps[m] - 2 * steps[m] * bits[m])

    core_peer, x_peer = flip(1), flip(2)

    def y_peer(d):
        return (tok, lax.rem(y + d, 4) * 4 + yx)

    def z_peer(d):
        return (xlo * 4 + lax.rem(z + d, 4), feat)

    xlo_peer = (lax.rem(tok + 4, 8), feat)

    def local_copy(src, dst, sem):
        return pltpu.make_async_copy(src, dst, sem)

    def remote(src, dst, s, r, dev):
        return pltpu.make_async_remote_copy(
            src_ref=src, dst_ref=dst, send_sem=s, recv_sem=r, device_id=dev, device_id_type=MESH
        )

    def rows(k, n=CT):
        return pl.ds(pl.multiple_of(k * n, n), n)

    def block_loads(m, slot):
        copies = []
        for i in range(2):
            for j in range(2):
                if m == 0:
                    r0, c0 = i * 128, j * 128
                else:
                    r0 = pl.multiple_of(lax.rem(bits[m] + i, 2) * 128, 128)
                    c0 = pl.multiple_of(lax.rem(bits[m] + j, 2) * 128, 128)
                copies.append(
                    local_copy(
                        bl.at[m, :, pl.ds(r0, 128), pl.ds(c0, 128)],
                        BS.at[pl.ds(4 * slot, 4), 2 * i + j],
                        bsem.at[m, 2 * i + j],
                    )
                )
        return copies

    def x_loads(k, to, at, sem):
        return [
            local_copy(x.at[pl.ds(k * CT, CT), pl.ds(h * 128, 128)], to(k, h), xsem.at[sem, k, h])
            for h in range(8)
        ]

    kt_load = local_copy(kv, KT, ktsem)
    kt_load.start()
    first_blocks = block_loads(0, 0)
    for cp in first_blocks:
        cp.start()
    x_copies = [x_loads(k, lambda k, h: XP.at[k // 2, k % 2, h], None, 0) for k in range(NC)]
    for cp in x_copies[0]:
        cp.start()
    second_blocks = block_loads(1, 1)
    for cp in second_blocks:
        cp.start()
    for k in range(1, NC):
        for cp in x_copies[k]:
            cp.start()

    def w_load(step):
        src = kw if step < 8 else vw
        return local_copy(src.at[pl.ds((step % 8) * 128, 128), :], ST.at[step % 2], stsem.at[step % 2])

    w_load(0).start()
    w_load(1).start()

    barrier = pltpu.get_barrier_semaphore()
    peers = [core_peer, x_peer, y_peer(1), y_peer(2), y_peer(3), z_peer(1), z_peer(2), z_peer(3), xlo_peer]
    for dev in peers:
        pl.semaphore_signal(barrier, inc=1, device_id=dev, device_id_type=MESH)

    for m in range(4):
        order = jnp.broadcast_to(ro[m : m + 1, :], (128, 128))
        hot = (lax.broadcasted_iota(jnp.int32, (128, 128), 0) == order).astype(F32)
        TT[m] = hot.astype(BF16)
        TS[m] = jnp.transpose(hot).astype(BF16)

    def prepare(m, slot, copies):
        for cp in copies:
            cp.wait()
        table = TS[m]

        def one(c, carry):
            for i in range(2):
                for j in range(2):
                    hi, lo = split(BS[4 * slot + c, 2 * i + j])
                    ph = jnp.dot(table, hi, preferred_element_type=F32)
                    p_lo = jnp.dot(table, lo, preferred_element_type=F32)
                    AH[m, c, i * 128 : (i + 1) * 128, j * 128 : (j + 1) * 128] = ph.astype(BF16)
                    AL[m, c, i * 128 : (i + 1) * 128, j * 128 : (j + 1) * 128] = p_lo.astype(BF16)
            return carry

        lax.fori_loop(0, 4, one, 0)

    prepare(0, 0, first_blocks)
    third_blocks = block_loads(2, 0)
    for cp in third_blocks:
        cp.start()

    pl.semaphore_wait(barrier, len(peers))

    def fwd_out(m, k):
        return remote(
            R.at[m - 1, 1 - bits[m], :, rows(k)], I.at[m - 1, :, rows(k)],
            ss.at[0, m - 1, 0, k], rs.at[0, m - 1, 0, k], flip(m),
        )

    def fwd_back(m, k):
        return remote(
            T.at[m - 1, :, rows(k)], R.at[m, bits[m], :, rows(k)],
            ss.at[0, m - 1, 1, k], rs.at[0, m - 1, 1, k], flip(m),
        )

    def bwd_out(m, k):
        return remote(
            G.at[m, 1 - bits[m], :, rows(k)], J.at[m - 1, :, rows(k)],
            ss.at[1, m - 1, 0, k], rs.at[1, m - 1, 0, k], flip(m),
        )

    def bwd_back(m, k):
        return remote(
            T.at[m - 1, :, rows(k)], G.at[m - 1, bits[m], :, rows(k)],
            ss.at[1, m - 1, 1, k], rs.at[1, m - 1, 1, k], flip(m),
        )

    def first_factor(k):
        for cp in x_copies[k]:
            cp.wait()
        for u in range(2):
            for c in range(2):
                h = 4 * u + 2 * c
                pair = jnp.concatenate([XP[k // 2, k % 2, h], XP[k // 2, k % 2, h + 1]], axis=1)
                hi, lo = split(pair)
                out = dot3(hi, lo, AH[0, 2 * u + c], AL[0, 2 * u + c])
                R[0, u, 2 * c, k * CT : (k + 1) * CT] = out[:, :128]
                R[0, u, 2 * c + 1, k * CT : (k + 1) * CT] = out[:, 128:]

    def fwd_factor(m, k):
        own = bits[m]

        def one(c, carry):
            pair = jnp.concatenate([R[m - 1, own, c, rows(k)], I[m - 1, c, rows(k)]], axis=1)
            hi, lo = split(pair)
            out = dot3(hi, lo, AH[m, c], AL[m, c])
            R[m, own, c, rows(k)] = out[:, :128]
            T[m - 1, c, rows(k)] = out[:, 128:]
            return carry

        lax.fori_loop(0, 4, one, 0)

    def bwd_factor(m, k):
        own = bits[m]

        def one(c, carry):
            pair = jnp.concatenate([G[m, own, c, rows(k)], J[m - 1, c, rows(k)]], axis=1)
            hi, lo = split(pair)
            out = dot3(hi, lo, AH[m, c], AL[m, c], 1, 1)
            G[m - 1, own, c, rows(k)] = out[:, :128]
            T[m - 1, c, rows(k)] = out[:, 128:]
            return carry

        lax.fori_loop(0, 4, one, 0)

    kt_load.wait()
    pair_copy = remote(KT, KP, kvs.at[0], kvr.at[0], core_peer)
    pair_copy.start()

    for k in range(NC):
        first_factor(k)
        fwd_out(1, k).start()

    pair_copy.wait_recv()
    lane = lax.broadcasted_iota(jnp.int32, (512, 128), 1)
    mine = (lane < 64) == (core == 0)
    GKV[core, chip] = jnp.where(mine, KT[...], pltpu.roll(KP[...], 64, 1))

    def gx(h):
        return remote(
            GKV.at[core, chip, rows(h, HT)], GKV.at[core, chip, rows(h, HT)],
            kvs.at[1 + h], kvr.at[1 + h], x_peer,
        )

    chip_x = chip + 1 - 2 * xhi

    def gy(d, h, far):
        tile = chip_x if far else chip
        return remote(
            GKV.at[core, tile, rows(h, HT)], GKV.at[core, tile, rows(h, HT)],
            gs.at[far, d - 1, h], gr.at[far, d - 1, h], y_peer(d),
        )

    def gc(h):
        return remote(
            GKV.at[core, :, rows(h, HT)], GKV.at[core, :, rows(h, HT)],
            kvs.at[3 + h], kvr.at[3 + h], core_peer,
        )

    for h in range(2):
        gx(h).start()
    for h in range(2):
        for d in (1, 3, 2):
            gy(d, h, 0).start()

    prepare(1, 1, second_blocks)
    fourth_blocks = block_loads(3, 1)
    for cp in fourth_blocks:
        cp.start()

    for k in range(NC):
        fwd_out(1, k).wait_recv()
        fwd_factor(1, k)
        fwd_back(1, k).start()

    prepare(2, 0, third_blocks)

    for k in range(NC):
        fwd_back(1, k).wait_recv()
        fwd_out(2, k).start()

    for h in range(2):
        gx(h).wait_recv()
        for d in (1, 3, 2):
            gy(d, h, 1).start()

    prepare(3, 1, fourth_blocks)

    for step in range(16):
        w_load(step).wait()
        s, base = step // 8, (step % 8) * 128

        def strip(i, carry, s=s, base=base, slot=step % 2):
            hi, lo = split(ST[slot, pl.ds(pl.multiple_of(i * 32, 32), 32), :])
            at = pl.ds(pl.multiple_of(base + i * 32, 32), 32)
            for q in range(4):
                WH[s, q, at, :] = hi[:, q * 256 : (q + 1) * 256]
                WL[s, q, at, :] = lo[:, q * 256 : (q + 1) * 256]
            return carry

        lax.fori_loop(0, 4, strip, 0)
        if step + 2 < 16:
            w_load(step + 2).start()

    x_again = [x_loads(k, lambda k, h: BS.at[2 * k + h // 4, h % 4], None, 1) for k in range(NC)]
    for group in x_again:
        for cp in group:
            cp.start()
    share = pl.ds(pl.multiple_of(tok * 32, 32), 32)
    adam_loads = [
        local_copy(mo, AD.at[0], adsem.at[0]),
        local_copy(se, AD.at[1], adsem.at[1]),
        local_copy(bl.at[:, :, share, :], AD.at[2], adsem.at[2]),
    ]
    for cp in adam_loads:
        cp.start()

    def gathered(h):
        for far in range(2):
            for d in (1, 3, 2):
                gy(d, h, far).wait_recv()
        gc(h).start()

    def upstream(h):
        gc(h).wait_recv()
        for s in range(2):
            for t in range(8):
                hi, lo = split(GKV[s, t, h * HT : (h + 1) * HT, :])
                LH[s, :, t * 128 : (t + 1) * 128] = hi
                LL[s, :, t * 128 : (t + 1) * 128] = lo
        for u in range(2):

            def one(n, carry, u=u):
                at = pl.ds(pl.multiple_of(u * 512 + n * 256, 256), 256)
                acc = None
                for s in range(2):
                    for q in range(4):
                        lh = LH[s, :, q * 256 : (q + 1) * 256]
                        ll = LL[s, :, q * 256 : (q + 1) * 256]
                        part = dot3(lh, ll, WH[s, q, at, :], WL[s, q, at, :], 1, 1)
                        acc = part if acc is None else acc + part
                G[3, u, 2 * n, h * HT : (h + 1) * HT] = acc[:, :128]
                G[3, u, 2 * n + 1, h * HT : (h + 1) * HT] = acc[:, 128:]
                return carry

            lax.fori_loop(0, 2, one, 0)
        for k in (2 * h, 2 * h + 1):
            bwd_out(3, k).start()

    def fwd_step(m, k):
        fwd_out(m, k).wait_recv()
        fwd_factor(m, k)
        fwd_back(m, k).start()

    def bwd_step(m, k):
        bwd_out(m, k).wait_recv()
        bwd_factor(m, k)
        bwd_back(m, k).start()

    def fwd_next(m, k):
        fwd_back(m - 1, k).wait_recv()
        fwd_out(m, k).start()

    def bwd_next(m, k):
        bwd_back(m + 1, k).wait_recv()
        bwd_out(m, k).start()

    fwd_step(2, 0)
    gathered(0)
    fwd_step(2, 1)
    upstream(0)
    fwd_step(2, 2)
    gathered(1)
    fwd_step(2, 3)
    upstream(1)
    for k in range(NC):
        bwd_step(3, k)
    for k in range(NC):
        fwd_next(3, k)

    def gradient(m):
        own = 0 if m == 0 else bits[m]

        def one(c, carry):
            total = None
            for t in range(2):
                if m == 0:
                    left = jnp.concatenate(
                        [
                            jnp.concatenate(
                                [BS[2 * k + lax.div(c, 2), 2 * lax.rem(c, 2) + i] for i in range(2)], axis=1
                            )
                            for k in (2 * t, 2 * t + 1)
                        ],
                        axis=0,
                    )
                    u, base = lax.div(c, 2), 2 * lax.rem(c, 2)
                    right = jnp.concatenate([G[0, u, base + i, t * HT : (t + 1) * HT] for i in range(2)], axis=1)
                else:
                    at = slice(t * HT, (t + 1) * HT)
                    left = jnp.concatenate([R[m - 1, own, c, at], I[m - 1, c, at]], axis=1)
                    right = jnp.concatenate([G[m, own, c, at], J[m - 1, c, at]], axis=1)
                lh, ll = split(left)
                rh, rl = split(right)
                part = dot3(lh, ll, rh, rl, 0, 0)
                total = part if total is None else total + part
            table = TT[m]
            for i in range(2):
                hi, lo = split(total[i * 128 : (i + 1) * 128])
                back = jnp.dot(table, hi, preferred_element_type=F32) + jnp.dot(
                    table, lo, preferred_element_type=F32
                )
                ii = i if m == 0 else lax.rem(own + i, 2)
                for j in range(2):
                    jj = j if m == 0 else lax.rem(own + j, 2)
                    for zz in range(4):
                        GO[m, zz, ii, c, jj] = back[zz * 32 : (zz + 1) * 32, j * 128 : (j + 1) * 128]
            return carry

        lax.fori_loop(0, 4, one, 0)
        for d in (1, 3, 2):
            z_send(m, d).start()

    def z_send(m, d):
        return remote(
            GO.at[m, lax.rem(z + d, 4)], GL.at[m, d - 1], zs.at[m, d - 1], zr.at[m, d - 1], z_peer(d)
        )

    def u_send(m):
        return remote(GO.at[m, z, 1 - xlo], XG.at[m], us.at[m], ur.at[m], xlo_peer)

    def z_sum(m):
        for d in (1, 3, 2):
            z_send(m, d).wait_recv()
        for side in (1 - xlo, xlo):
            GO[m, z, side] = GO[m, z, side] + GL[m, 0, side] + GL[m, 1, side] + GL[m, 2, side]
        u_send(m).start()

    def adam(m):
        u_send(m).wait_recv()

        def one(c, carry):
            for j in range(2):
                at = slice(j * 128, (j + 1) * 128)
                grad = GO[m, z, xlo, c, j] + XG[m, c, j]
                moment = beta_one * AD[0, m, c, :, at] + (1.0 - beta_one) * grad
                second = beta_two * AD[1, m, c, :, at] + (1.0 - beta_two) * grad * grad
                step = learn_rate * (moment / bias_one) / (jnp.sqrt(second / bias_two) + epsilon)
                AD[0, m, c, :, at] = moment
                AD[1, m, c, :, at] = second
                AD[2, m, c, :, at] = AD[2, m, c, :, at] - step
            return carry

        lax.fori_loop(0, 4, one, 0)
        for i, out in enumerate((nm, ns, nb)):
            result(m, i, out).start()

    def result(m, i, out):
        return local_copy(AD.at[i, m], out.at[m], osem.at[i, m])

    def p_core(k):
        return remote(
            XP.at[k % 2, 1 - core], GKV.at[0, :, rows(k)], ps.at[0, k], pr.at[0, k], core_peer
        )

    def p_y(k, d):
        yy = lax.rem(y + d, 4)
        return remote(
            XP.at[k % 2, core, pl.ds(2 * yy, 2)], YL.at[d - 1, k], ps.at[d, k], pr.at[d, k], y_peer(d)
        )

    def p_x(k):
        return remote(
            XP.at[k % 2, core, 2 * y + 1 - xhi], XL.at[k], ps.at[4, k], pr.at[4, k], x_peer
        )

    def p_last(k):
        return remote(FT.at[k], KP.at[rows(k)], ps.at[5, k], pr.at[5, k], core_peer)

    def project(k):
        if k >= 2:
            p_core(k - 2).wait_send()
            for d in (1, 3, 2):
                p_y(k - 2, d).wait_send()
            p_x(k - 2).wait_send()
        for u in range(2):
            for c in range(4):
                hi, lo = split(R[3, u, c, k * CT : (k + 1) * CT])
                at = slice((u * 4 + c) * 128, (u * 4 + c + 1) * 128)
                LH[0, :CT, at] = hi
                LL[0, :CT, at] = lo
        for s in range(2):

            def one(n, carry, s=s):
                out = dot3(LH[0, :CT, :], LL[0, :CT, :], WH[s, n], WL[s, n])
                XP[k % 2, s, 2 * n] = out[:, :128]
                XP[k % 2, s, 2 * n + 1] = out[:, 128:]
                return carry

            lax.fori_loop(0, 4, one, 0)
        p_core(k).start()

    def project_y(k):
        p_core(k).wait_recv()

        def one(t, carry):
            XP[k % 2, core, t] = XP[k % 2, core, t] + GKV[0, t, k * CT : (k + 1) * CT]
            return carry

        lax.fori_loop(0, 8, one, 0)
        for d in (1, 3, 2):
            p_y(k, d).start()

    def project_x(k):
        for d in (1, 3, 2):
            p_y(k, d).wait_recv()
        for side in (1 - xhi, xhi):
            at = 2 * y + side
            XP[k % 2, core, at] = XP[k % 2, core, at] + YL[0, k, side] + YL[1, k, side] + YL[2, k, side]
        p_x(k).start()

    def project_last(k):
        p_x(k).wait_recv()
        FT[k] = XP[k % 2, core, 2 * y + xhi] + XL[k]
        p_last(k).start()

    def project_out(k):
        p_last(k).wait_recv()
        at = slice(k * CT, (k + 1) * CT)
        key_tile = jnp.where(core == 0, FT[k], KP[at])
        value_tile = jnp.where(core == 0, KP[at], FT[k])
        key_tile = jnp.where(core == 0, key_tile, pltpu.roll(key_tile, 64, 1))
        value_tile = jnp.where(core == 0, value_tile, pltpu.roll(value_tile, 64, 1))
        ko[at, :] = key_tile[:, :64]
        vo[at, :] = value_tile[:, :64]

    def fwd_last(k):
        bwd_back(3, k).wait_send()
        fwd_step(3, k)

    def bwd_mid(k):
        fwd_back(2, k).wait_send()
        bwd_step(2, k)

    def bwd_low(k):
        fwd_back(1, k).wait_send()
        bwd_step(1, k)

    bwd_next(2, 0)
    bwd_next(2, 1)
    bwd_mid(0)
    bwd_next(2, 2)
    bwd_mid(1)
    bwd_next(2, 3)
    bwd_mid(2)
    fwd_last(0)
    for h in range(2):
        gx(h).wait_send()
        gc(h).wait_send()
        for far in range(2):
            for d in (1, 3, 2):
                gy(d, h, far).wait_send()
    bwd_next(1, 0)
    bwd_mid(3)
    fwd_last(1)
    bwd_low(0)
    bwd_next(1, 1)
    fwd_last(2)
    bwd_low(1)
    bwd_next(1, 2)
    fwd_last(3)
    bwd_low(2)
    gradient(3)
    gradient(2)
    pair_copy.wait_send()
    fwd_back(3, 0).wait_recv()
    project(0)
    bwd_next(1, 3)
    project_y(0)
    bwd_low(3)
    fwd_back(3, 1).wait_recv()
    project(1)
    for k in range(NC):
        bwd_back(1, k).wait_recv()
    gradient(1)
    for group in x_again:
        for cp in group:
            cp.wait()
    gradient(0)
    project_y(1)
    project_x(0)
    project_last(0)
    for cp in adam_loads:
        cp.wait()
    project_x(1)
    project_last(1)
    fwd_back(3, 2).wait_recv()
    project(2)
    fwd_back(3, 3).wait_recv()
    project_y(2)
    z_sum(3)
    project(3)
    z_sum(2)
    project_y(3)
    project_out(0)
    project_out(1)
    adam(3)
    adam(2)
    z_sum(1)
    project_x(2)
    project_last(2)
    z_sum(0)
    project_x(3)
    project_last(3)
    adam(1)
    adam(0)
    project_out(2)
    project_out(3)

    for m in (1, 2, 3):
        for k in range(NC):
            fwd_out(m, k).wait_send()
            bwd_out(m, k).wait_send()
    for k in range(NC):
        fwd_back(3, k).wait_send()
        bwd_back(2, k).wait_send()
        bwd_back(1, k).wait_send()
        p_last(k).wait_send()
    for k in (2, 3):
        p_core(k).wait_send()
        for d in (1, 3, 2):
            p_y(k, d).wait_send()
        p_x(k).wait_send()
    for m in range(4):
        for d in (1, 3, 2):
            z_send(m, d).wait_send()
        u_send(m).wait_send()
        for i, out in enumerate((nm, ns, nb)):
            result(m, i, out).wait()


def local(x, kw, vw, bl, ro, kg, vg, mo, se):
    kv = jnp.concatenate([kg, vg], axis=1)
    hbm = pl.BlockSpec(memory_space=pl.ANY)
    vmem = pl.BlockSpec(memory_space=pltpu.VMEM)
    dma = pltpu.SemaphoreType.DMA
    tile = (128, 128)
    scratch = [
        pltpu.VMEM((2, 2, 8) + tile, F32),
        pltpu.VMEM((2, 4, 1024, 256), BF16),
        pltpu.VMEM((2, 4, 1024, 256), BF16),
        pltpu.VMEM((4, 4, 256, 256), BF16),
        pltpu.VMEM((4, 4, 256, 256), BF16),
        pltpu.VMEM((4,) + tile, BF16),
        pltpu.VMEM((4,) + tile, BF16),
        pltpu.VMEM((2, 128, 1024), F32),
        pltpu.VMEM((8, 4) + tile, F32),
        pltpu.VMEM((4, 2, 4, 512, 128), F32),
        pltpu.VMEM((3, 4, 512, 128), F32),
        pltpu.VMEM((3, 4, 512, 128), F32),
        pltpu.VMEM((4, 2, 4, 512, 128), F32),
        pltpu.VMEM((3, 4, 512, 128), F32),
        pltpu.VMEM((2, 8, 512, 128), F32),
        pltpu.VMEM((512, 128), F32),
        pltpu.VMEM((512, 128), F32),
        pltpu.VMEM((2, 256, 1024), BF16),
        pltpu.VMEM((2, 256, 1024), BF16),
        pltpu.VMEM((3, 4, 2) + tile, F32),
        pltpu.VMEM((4,) + tile, F32),
        pltpu.VMEM((4,) + tile, F32),
        pltpu.VMEM((4, 4, 2, 4, 2, 32, 128), F32),
        pltpu.VMEM((4, 3, 2, 4, 2, 32, 128), F32),
        pltpu.VMEM((4, 4, 2, 32, 128), F32),
        pltpu.VMEM((3, 4, 4, 32, 256), F32),
        dma((4, 4)),
        dma((2, 4, 8)),
        dma((2,)),
        dma(()),
        dma((3,)),
        dma((3, 4)),
        dma((2, 3, 2, 4)),
        dma((2, 3, 2, 4)),
        dma((5,)),
        dma((5,)),
        dma((2, 3, 2)),
        dma((2, 3, 2)),
        dma((6, 4)),
        dma((6, 4)),
        dma((4, 3)),
        dma((4, 3)),
        dma((4,)),
        dma((4,)),
    ]
    share = jax.ShapeDtypeStruct((4, 4, 32, 256), F32)
    narrow = jax.ShapeDtypeStruct((512, 64), F32)
    return pl.pallas_call(
        kernel,
        out_shape=(narrow, narrow, share, share, share),
        in_specs=[hbm, hbm, hbm, hbm, vmem, hbm, hbm, hbm],
        out_specs=(vmem, vmem, hbm, hbm, hbm),
        scratch_shapes=scratch,
        compiler_params=pltpu.CompilerParams(
            collective_id=0, has_side_effects=True, vmem_limit_bytes=67043328
        ),
    )(x, kw, vw, bl, ro, kv, mo, se)


def solution(mesh):
    placed = (
        P("tok", "feat"),
        P("feat", None),
        P("feat", None),
        P(None, "feat", None, None),
        P(),
        P("tok", "feat"),
        P("tok", "feat"),
        P(None, "feat", "tok", None),
        P(None, "feat", "tok", None),
    )
    return jax.shard_map(
        local,
        mesh=mesh,
        in_specs=placed,
        out_specs=(
            P("tok", "feat"),
            P("tok", "feat"),
            P(None, "feat", "tok", None),
            P(None, "feat", "tok", None),
            P(None, "feat", "tok", None),
        ),
        check_vma=False,
    )
```

```python
import jax
import jax.numpy as jnp
from jax import lax
from jax.experimental import pallas as pl
from jax.experimental.pallas import tpu as pltpu
from jax.sharding import PartitionSpec as P

MESH = pl.DeviceIdType.MESH
F32 = jnp.float32
BF16 = jnp.bfloat16
beta_one = 0.9
beta_two = 0.95
learn_rate = 0.01
epsilon = 1e-08
bias_one = 1.0 - 0.9**10
bias_two = 1.0 - 0.95**10

ORDER = (
    ("W", 0), ("W", 1), ("T",), ("TY", 0), ("B", 1), ("B", 2), ("B", 0), ("C", 1), ("B", 3),
    ("W", 2), ("W", 3), ("C", 0), ("C", 3), ("X", 0), ("TY", 1), ("Q", 2), ("W", 4), ("W", 5),
    ("D", 1), ("Z", 0), ("W", 6), ("W", 7), ("X", 1), ("H", 0), ("HS", 0), ("Q", 3), ("Z", 1),
    ("HS", 1), ("D", 3), ("D", 0), ("I", 0), ("H", 1), ("I", 1), ("C", 2), ("HS", 3), ("J", 0),
    ("HS", 2), ("J", 1), ("K", 0), ("I", 3), ("K", 1), ("I", 2), ("G", 2, 0), ("L", 0), ("E", 1),
    ("E", 0), ("J", 3), ("M", 0), ("L", 1), ("J", 2), ("M", 1), ("G", 1, 0), ("K", 3), ("F", 1),
    ("D", 2), ("N", 0), ("K", 2), ("F", 0), ("E", 3), ("G", 2, 1), ("G", 3, 0), ("L", 3), ("P", 1),
    ("M", 3), ("PY", 1), ("P", 0), ("E", 2), ("L", 2), ("PY", 0), ("F", 3), ("S", 2), ("M", 2),
    ("G", 1, 1), ("N", 1), ("PX", 1), ("U", 2), ("F", 2), ("G", 3, 1), ("PX", 0), ("S", 1),
    ("SX",), ("PL", 1), ("P", 3), ("U", 1), ("PY", 3), ("PL", 0), ("P", 2), ("S", 3), ("PO", 1),
    ("PO", 0), ("PY", 2), ("U", 0), ("PX", 3), ("U", 3), ("PL", 3), ("PX", 2), ("PO", 3),
    ("PL", 2), ("PO", 2),
)

CT = 128
NC = 4
HT = 256


def split(v):
    hi = v.astype(BF16)
    lo = (v - hi.astype(F32)).astype(BF16)
    return hi, lo


def dims(ca, cb):
    return (((ca,), (cb,)), ((), ()))


def dot3(ah, al, bh, bl, ca=1, cb=0):
    d = dims(ca, cb)
    out = lax.dot_general(ah, bh, d, preferred_element_type=F32)
    out = out + lax.dot_general(ah, bl, d, preferred_element_type=F32)
    return out + lax.dot_general(al, bh, d, preferred_element_type=F32)


def kernel(
    x, kw, vw, bl, ro, kg, vg,
    go, kvo,
    XP, WH, WL, AH, AL, TT, TS, ST, BS, R, I, T, G, J, GKV, KT, KP, LH, LL, YL, XL, FT, GO, GL, XG, KV,
    bsem, xsem, stsem, ktsem, osem,
    ss, rs, kvs, kvr, gs, gr, ps, pr, zs, zr, us, ur,
):
    tok = lax.axis_index("tok")
    feat = lax.axis_index("feat")
    z = lax.rem(tok, 4)
    xlo = lax.div(tok, 4)
    core = lax.rem(feat, 2)
    xhi = lax.rem(lax.div(feat, 2), 2)
    y = lax.div(feat, 4)
    yhi = lax.div(feat, 8)
    yx = lax.rem(feat, 4)
    chip = lax.div(feat, 2)
    bits = [None, core, xhi, yhi]
    steps = [None, 1, 2, 8]

    def flip(m):
        return (tok, feat + steps[m] - 2 * steps[m] * bits[m])

    core_peer, x_peer = flip(1), flip(2)

    def y_peer(d):
        return (tok, lax.rem(y + d, 4) * 4 + yx)

    def z_peer(d):
        return (xlo * 4 + lax.rem(z + d, 4), feat)

    xlo_peer = (lax.rem(tok + 4, 8), feat)

    def local_copy(src, dst, sem):
        return pltpu.make_async_copy(src, dst, sem)

    def remote(src, dst, s, r, dev):
        return pltpu.make_async_remote_copy(
            src_ref=src, dst_ref=dst, send_sem=s, recv_sem=r, device_id=dev, device_id_type=MESH
        )

    def rows(k, n=CT):
        return pl.ds(pl.multiple_of(k * n, n), n)

    def block_loads(m, slot):
        copies = []
        for i in range(2):
            for j in range(2):
                if m == 0:
                    r0, c0 = i * 128, j * 128
                else:
                    r0 = pl.multiple_of(lax.rem(bits[m] + i, 2) * 128, 128)
                    c0 = pl.multiple_of(lax.rem(bits[m] + j, 2) * 128, 128)
                copies.append(
                    local_copy(
                        bl.at[m, :, pl.ds(r0, 128), pl.ds(c0, 128)],
                        BS.at[pl.ds(4 * slot, 4), 2 * i + j],
                        bsem.at[m, 2 * i + j],
                    )
                )
        return copies

    def x_loads(k, to, at, sem):
        return [
            local_copy(x.at[pl.ds(k * CT, CT), pl.ds(h * 128, 128)], to(k, h), xsem.at[sem, k, h])
            for h in range(8)
        ]

    kt_loads = [
        local_copy(kg, KV.at[pl.ds(0, 64)], ktsem.at[0]),
        local_copy(vg, KV.at[pl.ds(64, 64)], ktsem.at[1]),
    ]
    for cp in kt_loads:
        cp.start()
    first_blocks = block_loads(0, 0)
    for cp in first_blocks:
        cp.start()
    x_copies = [x_loads(k, lambda k, h: XP.at[k // 2, k % 2, h], None, 0) for k in range(NC)]
    for cp in x_copies[0]:
        cp.start()
    second_blocks = block_loads(1, 1)
    for cp in second_blocks:
        cp.start()
    for k in range(1, NC):
        for cp in x_copies[k]:
            cp.start()

    def w_load(step):
        src = kw if step < 8 else vw
        return local_copy(src.at[pl.ds((step % 8) * 128, 128), :], ST.at[step % 4], stsem.at[step % 4])

    for step in range(4):
        w_load(step).start()

    barrier = pltpu.get_barrier_semaphore()
    peers = [core_peer, x_peer, y_peer(1), y_peer(2), y_peer(3), z_peer(1), z_peer(2), z_peer(3), xlo_peer]
    for dev in peers:
        pl.semaphore_signal(barrier, inc=1, device_id=dev, device_id_type=MESH)

    for m in range(4):
        order = jnp.broadcast_to(ro[m : m + 1, :], (128, 128))
        hot = (lax.broadcasted_iota(jnp.int32, (128, 128), 0) == order).astype(F32)
        TT[m] = hot.astype(BF16)
        TS[m] = jnp.transpose(hot).astype(BF16)

    def prepare(m, slot, copies):
        for cp in copies:
            cp.wait()
        table = TS[m]

        def one(c, carry):
            for i in range(2):
                for j in range(2):
                    hi, lo = split(BS[4 * slot + c, 2 * i + j])
                    ph = jnp.dot(table, hi, preferred_element_type=F32)
                    p_lo = jnp.dot(table, lo, preferred_element_type=F32)
                    AH[m, c, i * 128 : (i + 1) * 128, j * 128 : (j + 1) * 128] = ph.astype(BF16)
                    AL[m, c, i * 128 : (i + 1) * 128, j * 128 : (j + 1) * 128] = p_lo.astype(BF16)
            return carry

        lax.fori_loop(0, 4, one, 0)

    prepare(0, 0, first_blocks)
    third_blocks = block_loads(2, 0)
    for cp in third_blocks:
        cp.start()

    def fwd_out(m, k):
        return remote(
            R.at[m - 1, 1 - bits[m], :, rows(k)], I.at[m - 1, :, rows(k)],
            ss.at[0, m - 1, 0, k], rs.at[0, m - 1, 0, k], flip(m),
        )

    def fwd_back(m, k):
        return remote(
            T.at[m - 1, :, rows(k)], R.at[m, bits[m], :, rows(k)],
            ss.at[0, m - 1, 1, k], rs.at[0, m - 1, 1, k], flip(m),
        )

    def bwd_out(m, k):
        return remote(
            G.at[m, 1 - bits[m], :, rows(k)], J.at[m - 1, :, rows(k)],
            ss.at[1, m - 1, 0, k], rs.at[1, m - 1, 0, k], flip(m),
        )

    def bwd_back(m, k):
        return remote(
            T.at[m - 1, :, rows(k)], G.at[m - 1, bits[m], :, rows(k)],
            ss.at[1, m - 1, 1, k], rs.at[1, m - 1, 1, k], flip(m),
        )

    def first_factor(k):
        for cp in x_copies[k]:
            cp.wait()
        for u in range(2):
            for c in range(2):
                h = 4 * u + 2 * c
                pair = jnp.concatenate([XP[k // 2, k % 2, h], XP[k // 2, k % 2, h + 1]], axis=1)
                hi, lo = split(pair)
                out = dot3(hi, lo, AH[0, 2 * u + c], AL[0, 2 * u + c])
                R[0, u, 2 * c, k * CT : (k + 1) * CT] = out[:, :128]
                R[0, u, 2 * c + 1, k * CT : (k + 1) * CT] = out[:, 128:]

    def fwd_factor(m, k):
        own = bits[m]

        def one(c, carry):
            pair = jnp.concatenate([R[m - 1, own, c, rows(k)], I[m - 1, c, rows(k)]], axis=1)
            hi, lo = split(pair)
            out = dot3(hi, lo, AH[m, c], AL[m, c])
            R[m, own, c, rows(k)] = out[:, :128]
            T[m - 1, c, rows(k)] = out[:, 128:]
            return carry

        lax.fori_loop(0, 4, one, 0)

    def bwd_factor(m, k):
        own = bits[m]

        def one(c, carry):
            pair = jnp.concatenate([G[m, own, c, rows(k)], J[m - 1, c, rows(k)]], axis=1)
            hi, lo = split(pair)
            out = dot3(hi, lo, AH[m, c], AL[m, c], 1, 1)
            G[m - 1, own, c, rows(k)] = out[:, :128]
            T[m - 1, c, rows(k)] = out[:, 128:]
            return carry

        lax.fori_loop(0, 4, one, 0)

    pair_copy = remote(KT, KP, kvs.at[0], kvr.at[0], core_peer)
    chip_x = chip + 1 - 2 * xhi

    def gx(h):
        return remote(
            GKV.at[core, chip, rows(h, HT)], GKV.at[core, chip, rows(h, HT)],
            kvs.at[1 + h], kvr.at[1 + h], x_peer,
        )

    def gy(d, h, far):
        tile = chip_x if far else chip
        return remote(
            GKV.at[core, tile, rows(h, HT)], GKV.at[core, tile, rows(h, HT)],
            gs.at[far, d - 1, h], gr.at[far, d - 1, h], y_peer(d),
        )

    def gc(h):
        return remote(
            GKV.at[core, :, rows(h, HT)], GKV.at[core, :, rows(h, HT)],
            kvs.at[3 + h], kvr.at[3 + h], core_peer,
        )

    def tiles_send():
        for cp in kt_loads:
            cp.wait()
        KT[...] = jnp.transpose(KV[...])

    def tiles():
        pair_copy.wait_recv()
        lane = lax.broadcasted_iota(jnp.int32, (512, 128), 1)
        mine = (lane < 64) == (core == 0)
        GKV[core, chip] = jnp.where(mine, KT[...], pltpu.roll(KP[...], 64, 1))
        for h in range(2):
            gx(h).start()

    def gather_near(h):
        for d in (1, 3, 2):
            gy(d, h, 0).start()

    def gather_far(h):
        gx(h).wait_recv()
        for d in (1, 3, 2):
            gy(d, h, 1).start()

    def fwd_first(k):
        fwd_out(1, k).wait_recv()
        fwd_factor(1, k)
        fwd_back(1, k).start()

    def weights(part):
        for step in range(2 * part, 2 * part + 2):
            w_load(step).wait()
            s, base = step // 8, (step % 8) * 128

            def strip(i, carry, s=s, base=base, slot=step % 4):
                hi, lo = split(ST[slot, pl.ds(pl.multiple_of(i * 32, 32), 32), :])
                at = pl.ds(pl.multiple_of(base + i * 32, 32), 32)
                for q in range(4):
                    WH[s, q, at, :] = hi[:, q * 256 : (q + 1) * 256]
                    WL[s, q, at, :] = lo[:, q * 256 : (q + 1) * 256]
                return carry

            lax.fori_loop(0, 4, strip, 0)
            if step + 4 < 16:
                w_load(step + 4).start()

    x_again = [x_loads(k, lambda k, h: BS.at[2 * k + h // 4, h % 4], None, 1) for k in range(NC)]

    def gathered(h):
        for far in range(2):
            for d in (1, 3, 2):
                gy(d, h, far).wait_recv()
        gc(h).start()

    def upstream(h):
        gc(h).wait_recv()
        for s in range(2):
            for t in range(8):
                hi, lo = split(GKV[s, t, h * HT : (h + 1) * HT, :])
                LH[s, :, t * 128 : (t + 1) * 128] = hi
                LL[s, :, t * 128 : (t + 1) * 128] = lo
        for u in range(2):

            def one(n, carry, u=u):
                at = pl.ds(pl.multiple_of(u * 512 + n * 256, 256), 256)
                acc = None
                for s in range(2):
                    for q in range(4):
                        lh = LH[s, :, q * 256 : (q + 1) * 256]
                        ll = LL[s, :, q * 256 : (q + 1) * 256]
                        part = dot3(lh, ll, WH[s, q, at, :], WL[s, q, at, :], 1, 1)
                        acc = part if acc is None else acc + part
                G[3, u, 2 * n, h * HT : (h + 1) * HT] = acc[:, :128]
                G[3, u, 2 * n + 1, h * HT : (h + 1) * HT] = acc[:, 128:]
                return carry

            lax.fori_loop(0, 2, one, 0)

    def fwd_step(m, k):
        fwd_out(m, k).wait_recv()
        fwd_factor(m, k)
        fwd_back(m, k).start()

    def bwd_step(m, k):
        bwd_out(m, k).wait_recv()
        bwd_factor(m, k)
        bwd_back(m, k).start()

    def fwd_next(m, k):
        fwd_back(m - 1, k).wait_recv()
        fwd_out(m, k).start()

    def bwd_next(m, k):
        bwd_back(m + 1, k).wait_recv()
        bwd_out(m, k).start()

    def gradient(m, t):
        own = 0 if m == 0 else bits[m]

        def one(c, carry):
            if m == 0:
                left = jnp.concatenate(
                    [
                        jnp.concatenate(
                            [BS[2 * k + lax.div(c, 2), 2 * lax.rem(c, 2) + i] for i in range(2)], axis=1
                        )
                        for k in (2 * t, 2 * t + 1)
                    ],
                    axis=0,
                )
                u, base = lax.div(c, 2), 2 * lax.rem(c, 2)
                right = jnp.concatenate([G[0, u, base + i, t * HT : (t + 1) * HT] for i in range(2)], axis=1)
            else:
                at = slice(t * HT, (t + 1) * HT)
                left = jnp.concatenate([R[m - 1, own, c, at], I[m - 1, c, at]], axis=1)
                right = jnp.concatenate([G[m, own, c, at], J[m - 1, c, at]], axis=1)
            lh, ll = split(left)
            rh, rl = split(right)
            total = dot3(lh, ll, rh, rl, 0, 0)
            table = TT[m]
            for i in range(2):
                hi, lo = split(total[i * 128 : (i + 1) * 128])
                back = jnp.dot(table, hi, preferred_element_type=F32) + jnp.dot(
                    table, lo, preferred_element_type=F32
                )
                ii = i if m == 0 else lax.rem(own + i, 2)
                for j in range(2):
                    jj = j if m == 0 else lax.rem(own + j, 2)
                    for zz in range(4):
                        piece = back[zz * 32 : (zz + 1) * 32, j * 128 : (j + 1) * 128]
                        GO[m, zz, ii, c, jj] = piece if t == 0 else GO[m, zz, ii, c, jj] + piece
            return carry

        lax.fori_loop(0, 4, one, 0)
        if t == 1 and m == 0:
            for zz in range(4):
                x_first(zz).start()
        if t == 1 and m > 0:
            for d in (1, 3, 2):
                z_send(m, d).start()

    def x_land(zz):
        return XG.at[0] if zz == 3 else GL.at[0, zz, 1]

    def x_first(zz):
        return remote(
            GO.at[0, zz, 1 - xlo], x_land(zz), zs.at[4, zz], zr.at[4, zz], xlo_peer
        )

    def z_last(d):
        return remote(
            GO.at[0, lax.rem(z + d, 4), xlo], GL.at[0, d - 1, 0], zs.at[0, d - 1], zr.at[0, d - 1], z_peer(d)
        )

    def x_sum():
        for zz in range(4):
            x_first(zz).wait_recv()
            GO[0, zz, xlo] = GO[0, zz, xlo] + x_land(zz)[...]
        for d in (1, 3, 2):
            z_last(d).start()

    def z_send(m, d):
        return remote(
            GO.at[m, lax.rem(z + d, 4)], GL.at[m, d - 1], zs.at[m, d - 1], zr.at[m, d - 1], z_peer(d)
        )

    def u_send(m):
        return remote(GO.at[m, z, 1 - xlo], XG.at[m], us.at[m], ur.at[m], xlo_peer)

    def z_sum(m):
        for d in (1, 3, 2):
            z_send(m, d).wait_recv()
        for side in (1 - xlo, xlo):
            GO[m, z, side] = GO[m, z, side] + GL[m, 0, side] + GL[m, 1, side] + GL[m, 2, side]
        u_send(m).start()

    def share_sum(m):
        if m == 0:
            for d in (1, 3, 2):
                z_last(d).wait_recv()
            GO[0, z, xlo] = GO[0, z, xlo] + GL[0, 0, 0] + GL[0, 1, 0] + GL[0, 2, 0]
        else:
            u_send(m).wait_recv()
            GO[m, z, xlo] = GO[m, z, xlo] + XG[m]
        result(m).start()

    def result(m):
        return local_copy(GO.at[m, z, xlo], go.at[m], osem.at[m])

    def kv_result():
        return local_copy(KV, kvo, osem.at[4])

    def p_core(k):
        return remote(
            XP.at[k % 2, 1 - core], GKV.at[0, :, rows(k)], ps.at[0, k], pr.at[0, k], core_peer
        )

    def p_y(k, d):
        yy = lax.rem(y + d, 4)
        return remote(
            XP.at[k % 2, core, pl.ds(2 * yy, 2)], YL.at[d - 1, k], ps.at[d, k], pr.at[d, k], y_peer(d)
        )

    def p_x(k):
        return remote(
            XP.at[k % 2, core, 2 * y + 1 - xhi], XL.at[k], ps.at[4, k], pr.at[4, k], x_peer
        )

    def p_last(k):
        return remote(FT.at[k], KP.at[rows(k)], ps.at[5, k], pr.at[5, k], core_peer)

    def project(k):
        if k >= 2:
            p_core(k - 2).wait_send()
            for d in (1, 3, 2):
                p_y(k - 2, d).wait_send()
            p_x(k - 2).wait_send()
        for u in range(2):
            for c in range(4):
                hi, lo = split(R[3, u, c, k * CT : (k + 1) * CT])
                at = slice((u * 4 + c) * 128, (u * 4 + c + 1) * 128)
                LH[0, :CT, at] = hi
                LL[0, :CT, at] = lo
        for s in range(2):

            def one(n, carry, s=s):
                out = dot3(LH[0, :CT, :], LL[0, :CT, :], WH[s, n], WL[s, n])
                XP[k % 2, s, 2 * n] = out[:, :128]
                XP[k % 2, s, 2 * n + 1] = out[:, 128:]
                return carry

            lax.fori_loop(0, 4, one, 0)
        p_core(k).start()

    def project_y(k):
        p_core(k).wait_recv()

        def one(t, carry):
            XP[k % 2, core, t] = XP[k % 2, core, t] + GKV[0, t, k * CT : (k + 1) * CT]
            return carry

        lax.fori_loop(0, 8, one, 0)
        for d in (1, 3, 2):
            p_y(k, d).start()

    def project_x(k):
        for d in (1, 3, 2):
            p_y(k, d).wait_recv()
        for side in (1 - xhi, xhi):
            at = 2 * y + side
            XP[k % 2, core, at] = XP[k % 2, core, at] + YL[0, k, side] + YL[1, k, side] + YL[2, k, side]
        p_x(k).start()

    def project_last(k):
        p_x(k).wait_recv()
        FT[k] = XP[k % 2, core, 2 * y + xhi] + XL[k]
        p_last(k).start()

    def project_out(k):
        p_last(k).wait_recv()
        at = slice(k * CT, (k + 1) * CT)
        key_tile = jnp.where(core == 0, FT[k], KP[at])
        value_tile = jnp.where(core == 0, KP[at], FT[k])
        key_tile = jnp.transpose(key_tile)
        value_tile = jnp.transpose(value_tile)
        KV[:64, at] = jnp.where(core == 0, key_tile[:64], key_tile[64:])
        KV[64:, at] = jnp.where(core == 0, value_tile[:64], value_tile[64:])

    def fwd_last(k):
        bwd_back(3, k).wait_send()
        fwd_step(3, k)

    def bwd_mid(k):
        fwd_back(2, k).wait_send()
        bwd_step(2, k)

    def bwd_low(k):
        fwd_back(1, k).wait_send()
        bwd_step(1, k)

    def gather_done():
        for h in range(2):
            gx(h).wait_send()
            gc(h).wait_send()
            for far in range(2):
                for d in (1, 3, 2):
                    gy(d, h, far).wait_send()

    def bwd_low_out(k):
        if k == 0:
            gather_done()
        bwd_next(1, k)

    def bwd_grad0(t):
        for k in (2 * t, 2 * t + 1):
            bwd_back(1, k).wait_recv()
            for cp in x_again[k]:
                cp.wait()
        gradient(0, t)

    def project_in(k):
        fwd_back(3, k).wait_recv()
        project(k)

    def late_prepare(m):
        prepare(m, m % 2, third_blocks if m == 2 else fourth_blocks)
        if m == 3:
            for group in x_again:
                for cp in group:
                    cp.start()

    steps_of = {
        "Q": late_prepare,
        "T": tiles,
        "X": gather_far,
        "TY": gather_near,
        "Z": gathered,
        "W": weights,
        "H": upstream,
        "HS": lambda k: bwd_out(3, k).start(),
        "B": fwd_first,
        "C": lambda k: fwd_next(2, k),
        "D": lambda k: fwd_step(2, k),
        "E": lambda k: fwd_next(3, k),
        "F": fwd_last,
        "I": lambda k: bwd_step(3, k),
        "J": lambda k: bwd_next(2, k),
        "K": bwd_mid,
        "L": bwd_low_out,
        "M": bwd_low,
        "G": gradient,
        "N": bwd_grad0,
        "P": project_in,
        "PY": project_y,
        "PX": project_x,
        "PL": project_last,
        "PO": project_out,
        "S": z_sum,
        "SX": x_sum,
        "U": share_sum,
    }

    tiles_send()
    for k in range(NC):
        first_factor(k)
    prepare(1, 1, second_blocks)
    fourth_blocks = block_loads(3, 1)
    for cp in fourth_blocks:
        cp.start()
    pl.semaphore_wait(barrier, len(peers))
    pair_copy.start()
    for k in range(NC):
        fwd_out(1, k).start()

    for name, *args in ORDER:
        steps_of[name](*args)
    kv_result().start()

    for m in (1, 2, 3):
        for k in range(NC):
            fwd_out(m, k).wait_send()
            bwd_out(m, k).wait_send()
    for k in range(NC):
        fwd_back(3, k).wait_send()
        bwd_back(2, k).wait_send()
        bwd_back(1, k).wait_send()
        p_last(k).wait_send()
    for k in (2, 3):
        p_core(k).wait_send()
        for d in (1, 3, 2):
            p_y(k, d).wait_send()
        p_x(k).wait_send()
    pair_copy.wait_send()
    for m in range(4):
        for d in (1, 3, 2):
            (z_send(m, d) if m else z_last(d)).wait_send()
        if m:
            u_send(m).wait_send()
        result(m).wait()
    for zz in range(4):
        x_first(zz).wait_send()
    kv_result().wait()


def finish(g, kv, mo, se, bl, ko, vo, nb, nm, ns, GV, KB, A, isem, jsem, osem):
    tok = lax.axis_index("tok")
    share = pl.ds(pl.multiple_of(tok * 32, 32), 32)
    copy = pltpu.make_async_copy

    def loads(m):
        return [
            copy(g.at[m], GV.at[m], isem.at[0, m]),
            copy(mo.at[m], A.at[0, m], isem.at[1, m]),
            copy(se.at[m], A.at[1, m], isem.at[2, m]),
            copy(bl.at[m, :, share, :], A.at[2, m], isem.at[3, m]),
        ]

    def stores(m):
        return [copy(A.at[i, m], out.at[m], osem.at[i, m]) for i, out in enumerate((nm, ns, nb))]

    kv_load = copy(kv, KB, jsem.at[0])
    kv_load.start()
    every = [loads(m) for m in range(4)]
    for group in every:
        for cp in group:
            cp.start()
    kv_load.wait()
    kv_stores = [
        copy(KB.at[pl.ds(0, 64)], ko, jsem.at[1]),
        copy(KB.at[pl.ds(64, 64)], vo, jsem.at[2]),
    ]
    for cp in kv_stores:
        cp.start()
    for m in range(4):
        for cp in every[m]:
            cp.wait()
        for c in range(4):
            for j in range(2):
                at = slice(j * 128, (j + 1) * 128)
                grad = GV[m, c, j]
                moment = beta_one * A[0, m, c, :, at] + (1.0 - beta_one) * grad
                second = beta_two * A[1, m, c, :, at] + (1.0 - beta_two) * grad * grad
                step = learn_rate * (moment / bias_one) / (jnp.sqrt(second / bias_two) + epsilon)
                A[0, m, c, :, at] = moment
                A[1, m, c, :, at] = second
                A[2, m, c, :, at] = A[2, m, c, :, at] - step
        for cp in stores(m):
            cp.start()
    for m in range(4):
        for cp in stores(m):
            cp.wait()
    for cp in kv_stores:
        cp.wait()


def local(x, kw, vw, bl, ro, kg, vg, mo, se):
    hbm = pl.BlockSpec(memory_space=pl.ANY)
    vmem = pl.BlockSpec(memory_space=pltpu.VMEM)
    dma = pltpu.SemaphoreType.DMA
    tile = (128, 128)
    scratch = [
        pltpu.VMEM((2, 2, 8) + tile, F32),
        pltpu.VMEM((2, 4, 1024, 256), BF16),
        pltpu.VMEM((2, 4, 1024, 256), BF16),
        pltpu.VMEM((4, 4, 256, 256), BF16),
        pltpu.VMEM((4, 4, 256, 256), BF16),
        pltpu.VMEM((4,) + tile, BF16),
        pltpu.VMEM((4,) + tile, BF16),
        pltpu.VMEM((4, 128, 1024), F32),
        pltpu.VMEM((8, 4) + tile, F32),
        pltpu.VMEM((4, 2, 4, 512, 128), F32),
        pltpu.VMEM((3, 4, 512, 128), F32),
        pltpu.VMEM((3, 4, 512, 128), F32),
        pltpu.VMEM((4, 2, 4, 512, 128), F32),
        pltpu.VMEM((3, 4, 512, 128), F32),
        pltpu.VMEM((2, 8, 512, 128), F32),
        pltpu.VMEM((512, 128), F32),
        pltpu.VMEM((512, 128), F32),
        pltpu.VMEM((2, 256, 1024), BF16),
        pltpu.VMEM((2, 256, 1024), BF16),
        pltpu.VMEM((3, 4, 2) + tile, F32),
        pltpu.VMEM((4,) + tile, F32),
        pltpu.VMEM((4,) + tile, F32),
        pltpu.VMEM((4, 4, 2, 4, 2, 32, 128), F32),
        pltpu.VMEM((4, 3, 2, 4, 2, 32, 128), F32),
        pltpu.VMEM((4, 4, 2, 32, 128), F32),
        pltpu.VMEM((128, 512), F32),
        dma((4, 4)),
        dma((2, 4, 8)),
        dma((4,)),
        dma((2,)),
        dma((5,)),
        dma((2, 3, 2, 4)),
        dma((2, 3, 2, 4)),
        dma((5,)),
        dma((5,)),
        dma((2, 3, 2)),
        dma((2, 3, 2)),
        dma((6, 4)),
        dma((6, 4)),
        dma((5, 4)),
        dma((5, 4)),
        dma((4,)),
        dma((4,)),
    ]
    share = jax.ShapeDtypeStruct((4, 4, 32, 256), F32)
    narrow = jax.ShapeDtypeStruct((64, 512), F32)
    grads, kv = pl.pallas_call(
        kernel,
        out_shape=(
            jax.ShapeDtypeStruct((4, 4, 2, 32, 128), F32),
            jax.ShapeDtypeStruct((128, 512), F32),
        ),
        in_specs=[hbm, hbm, hbm, hbm, vmem, hbm, hbm],
        out_specs=(hbm, hbm),
        scratch_shapes=scratch,
        compiler_params=pltpu.CompilerParams(
            collective_id=0, has_side_effects=True, vmem_limit_bytes=67043328
        ),
    )(x, kw, vw, bl, ro, kg.T, vg.T)
    ko, vo, nb, nm, ns = pl.pallas_call(
        finish,
        out_shape=(narrow, narrow, share, share, share),
        in_specs=[hbm] * 5,
        out_specs=(hbm,) * 5,
        scratch_shapes=[
            pltpu.VMEM((4, 4, 2, 32, 128), F32),
            pltpu.VMEM((128, 512), F32),
            pltpu.VMEM((3, 4, 4, 32, 256), F32),
            dma((4, 4)),
            dma((3,)),
            dma((3, 4)),
        ],
    )(grads, kv, mo, se, bl)
    return ko.T, vo.T, nb, nm, ns


def solution(mesh):
    placed = (
        P("tok", "feat"),
        P("feat", None),
        P("feat", None),
        P(None, "feat", None, None),
        P(),
        P("tok", "feat"),
        P("tok", "feat"),
        P(None, "feat", "tok", None),
        P(None, "feat", "tok", None),
    )
    return jax.shard_map(
        local,
        mesh=mesh,
        in_specs=placed,
        out_specs=(
            P("tok", "feat"),
            P("tok", "feat"),
            P(None, "feat", "tok", None),
            P(None, "feat", "tok", None),
            P(None, "feat", "tok", None),
        ),
        check_vma=False,
    )
```

```python
import jax
import jax.numpy as jnp
from jax import lax
from jax.experimental import pallas as pl
from jax.experimental.pallas import tpu as pltpu
from jax.sharding import PartitionSpec as P

MESH = pl.DeviceIdType.MESH
F32 = jnp.float32
BF16 = jnp.bfloat16
beta_one = 0.9
beta_two = 0.95
learn_rate = 0.01
epsilon = 1e-08
bias_one = 1.0 - 0.9**10
bias_two = 1.0 - 0.95**10

ORDER = (
    ("Q", 2), ("T",), ("TY", 0), ("W", 0), ("W", 1), ("B", 3), ("B", 1), ("B", 0), ("W", 2),
    ("W", 3), ("C", 3), ("X", 0), ("W", 4), ("X", 1), ("C", 0), ("Q", 3), ("C", 1), ("W", 5),
    ("D", 3), ("TY", 1), ("W", 6), ("W", 7), ("Z", 0), ("H", 0), ("HS", 0), ("B", 2), ("D", 0),
    ("C", 2), ("Z", 1), ("D", 1), ("HS", 1), ("I", 0), ("H", 1), ("I", 1), ("J", 0), ("HS", 3),
    ("J", 1), ("HS", 2), ("K", 0), ("I", 3), ("K", 1), ("I", 2), ("L", 0), ("J", 3), ("E", 1),
    ("M", 0), ("G", 2, 0), ("E", 0), ("L", 1), ("J", 2), ("M", 1), ("G", 1, 0), ("K", 3), ("F", 1),
    ("N", 0), ("D", 2), ("K", 2), ("F", 0), ("G", 2, 1), ("E", 3), ("L", 3), ("P", 1), ("M", 3),
    ("E", 2), ("PY", 1), ("P", 0), ("L", 2), ("PY", 0), ("F", 3), ("M", 2), ("S", 2), ("G", 1, 1),
    ("PX", 1), ("N", 1), ("F", 2), ("G", 3, 0), ("PX", 0), ("G", 3, 1), ("U", 2), ("PL", 1),
    ("P", 3), ("PO", 1), ("PY", 3), ("S", 1), ("PL", 0), ("P", 2), ("SX", 0), ("PY", 2), ("S", 3),
    ("U", 1), ("U", 0), ("PO", 0), ("PL", 2), ("PL", 3), ("PO", 3), ("PO", 2), ("U", 3),
)

CT = 128
NC = 4
HT = 256


def split(v):
    hi = v.astype(BF16)
    lo = (v - hi.astype(F32)).astype(BF16)
    return hi, lo


def dims(ca, cb):
    return (((ca,), (cb,)), ((), ()))


def dot3(ah, al, bh, bl, ca=1, cb=0):
    d = dims(ca, cb)
    out = lax.dot_general(ah, bh, d, preferred_element_type=F32)
    out = out + lax.dot_general(ah, bl, d, preferred_element_type=F32)
    return out + lax.dot_general(al, bh, d, preferred_element_type=F32)


def kernel(
    x, kw, vw, bl, ro, kg, vg,
    go, kvo,
    XP, WH, WL, AH, AL, TT, TS, ST, BS, R, I, T, G, J, GKV, KT, KP, LH, LL, YL, XL, DL, FT, GO, GL, XG, KV,
    bsem, xsem, stsem, ktsem, osem,
    ss, rs, kvs, kvr, gs, gr, ps, pr, zs, zr, us, ur,
):
    tok = lax.axis_index("tok")
    feat = lax.axis_index("feat")
    z = lax.rem(tok, 4)
    xlo = lax.div(tok, 4)
    core = lax.rem(feat, 2)
    xhi = lax.rem(lax.div(feat, 2), 2)
    y = lax.div(feat, 4)
    yhi = lax.div(feat, 8)
    yx = lax.rem(feat, 4)
    chip = xhi * 4 + y
    bits = [None, core, xhi, yhi]
    steps = [None, 1, 2, 8]

    def flip(m):
        return (tok, feat + steps[m] - 2 * steps[m] * bits[m])

    core_peer, x_peer = flip(1), flip(2)

    def y_peer(d):
        return (tok, lax.rem(y + d, 4) * 4 + yx)

    def xy_peer(d):
        return (tok, lax.rem(y + d, 4) * 4 + yx + 2 - 4 * xhi)

    def z_peer(d):
        return (xlo * 4 + lax.rem(z + d, 4), feat)

    xlo_peer = (lax.rem(tok + 4, 8), feat)

    def local_copy(src, dst, sem):
        return pltpu.make_async_copy(src, dst, sem)

    def remote(src, dst, s, r, dev):
        return pltpu.make_async_remote_copy(
            src_ref=src, dst_ref=dst, send_sem=s, recv_sem=r, device_id=dev, device_id_type=MESH
        )

    def rows(k, n=CT):
        return pl.ds(pl.multiple_of(k * n, n), n)

    def block_loads(m, slot):
        copies = []
        for i in range(2):
            for j in range(2):
                if m == 0:
                    r0, c0 = i * 128, j * 128
                else:
                    r0 = pl.multiple_of(lax.rem(bits[m] + i, 2) * 128, 128)
                    c0 = pl.multiple_of(lax.rem(bits[m] + j, 2) * 128, 128)
                copies.append(
                    local_copy(
                        bl.at[m, :, pl.ds(r0, 128), pl.ds(c0, 128)],
                        BS.at[pl.ds(4 * slot, 4), 2 * i + j],
                        bsem.at[m, 2 * i + j],
                    )
                )
        return copies

    def x_loads(k, to, at, sem):
        return [
            local_copy(x.at[pl.ds(k * CT, CT), pl.ds(h * 128, 128)], to(k, h), xsem.at[sem, k, h])
            for h in range(8)
        ]

    kt_loads = [
        local_copy(kg, KV.at[pl.ds(0, 64)], ktsem.at[0]),
        local_copy(vg, KV.at[pl.ds(64, 64)], ktsem.at[1]),
    ]
    for cp in kt_loads:
        cp.start()
    first_blocks = block_loads(0, 0)
    for cp in first_blocks:
        cp.start()
    x_copies = [x_loads(k, lambda k, h: XP.at[k // 2, k % 2, h], None, 0) for k in range(NC)]
    for cp in x_copies[0]:
        cp.start()
    second_blocks = block_loads(1, 1)
    for cp in second_blocks:
        cp.start()
    for k in range(1, NC):
        for cp in x_copies[k]:
            cp.start()

    def w_load(step):
        src = kw if step < 8 else vw
        return local_copy(src.at[pl.ds((step % 8) * 128, 128), :], ST.at[step % 4], stsem.at[step % 4])

    for step in range(4):
        w_load(step).start()

    barrier = pltpu.get_barrier_semaphore()
    peers = [core_peer, x_peer, y_peer(1), y_peer(2), y_peer(3), z_peer(1), z_peer(2), z_peer(3), xlo_peer]
    peers += [xy_peer(1), xy_peer(2), xy_peer(3)]
    for dev in peers:
        pl.semaphore_signal(barrier, inc=1, device_id=dev, device_id_type=MESH)

    for m in range(4):
        order = jnp.broadcast_to(ro[m : m + 1, :], (128, 128))
        hot = (lax.broadcasted_iota(jnp.int32, (128, 128), 0) == order).astype(F32)
        TT[m] = hot.astype(BF16)
        TS[m] = jnp.transpose(hot).astype(BF16)

    def prepare(m, slot, copies):
        for cp in copies:
            cp.wait()
        table = TS[m]

        def one(c, carry):
            for i in range(2):
                for j in range(2):
                    hi, lo = split(BS[4 * slot + c, 2 * i + j])
                    ph = jnp.dot(table, hi, preferred_element_type=F32)
                    p_lo = jnp.dot(table, lo, preferred_element_type=F32)
                    AH[m, c, i * 128 : (i + 1) * 128, j * 128 : (j + 1) * 128] = ph.astype(BF16)
                    AL[m, c, i * 128 : (i + 1) * 128, j * 128 : (j + 1) * 128] = p_lo.astype(BF16)
            return carry

        lax.fori_loop(0, 4, one, 0)

    prepare(0, 0, first_blocks)
    third_blocks = block_loads(2, 0)
    for cp in third_blocks:
        cp.start()

    def fwd_out(m, k):
        return remote(
            R.at[m - 1, 1 - bits[m], :, rows(k)], I.at[m - 1, :, rows(k)],
            ss.at[0, m - 1, 0, k], rs.at[0, m - 1, 0, k], flip(m),
        )

    def fwd_back(m, k):
        return remote(
            T.at[m - 1, :, rows(k)], R.at[m, bits[m], :, rows(k)],
            ss.at[0, m - 1, 1, k], rs.at[0, m - 1, 1, k], flip(m),
        )

    def bwd_out(m, k):
        return remote(
            G.at[m, 1 - bits[m], :, rows(k)], J.at[m - 1, :, rows(k)],
            ss.at[1, m - 1, 0, k], rs.at[1, m - 1, 0, k], flip(m),
        )

    def bwd_back(m, k):
        return remote(
            T.at[m - 1, :, rows(k)], G.at[m - 1, bits[m], :, rows(k)],
            ss.at[1, m - 1, 1, k], rs.at[1, m - 1, 1, k], flip(m),
        )

    def first_factor(k):
        for cp in x_copies[k]:
            cp.wait()
        for u in range(2):
            for c in range(2):
                h = 4 * u + 2 * c
                pair = jnp.concatenate([XP[k // 2, k % 2, h], XP[k // 2, k % 2, h + 1]], axis=1)
                hi, lo = split(pair)
                out = dot3(hi, lo, AH[0, 2 * u + c], AL[0, 2 * u + c])
                R[0, u, 2 * c, k * CT : (k + 1) * CT] = out[:, :128]
                R[0, u, 2 * c + 1, k * CT : (k + 1) * CT] = out[:, 128:]

    def fwd_factor(m, k):
        own = bits[m]

        def one(c, carry):
            pair = jnp.concatenate([R[m - 1, own, c, rows(k)], I[m - 1, c, rows(k)]], axis=1)
            hi, lo = split(pair)
            out = dot3(hi, lo, AH[m, c], AL[m, c])
            R[m, own, c, rows(k)] = out[:, :128]
            T[m - 1, c, rows(k)] = out[:, 128:]
            return carry

        lax.fori_loop(0, 4, one, 0)

    def bwd_factor(m, k):
        own = bits[m]

        def one(c, carry):
            pair = jnp.concatenate([G[m, own, c, rows(k)], J[m - 1, c, rows(k)]], axis=1)
            hi, lo = split(pair)
            out = dot3(hi, lo, AH[m, c], AL[m, c], 1, 1)
            G[m - 1, own, c, rows(k)] = out[:, :128]
            T[m - 1, c, rows(k)] = out[:, 128:]
            return carry

        lax.fori_loop(0, 4, one, 0)

    pair_copy = remote(KT, KP, kvs.at[0], kvr.at[0], core_peer)
    chip_x = (1 - xhi) * 4 + y

    def gx(h):
        return remote(
            GKV.at[core, chip, rows(h, HT)], GKV.at[core, chip, rows(h, HT)],
            kvs.at[1 + h], kvr.at[1 + h], x_peer,
        )

    def gy(d, h, far):
        tile = chip_x if far else chip
        return remote(
            GKV.at[core, tile, rows(h, HT)], GKV.at[core, tile, rows(h, HT)],
            gs.at[far, d - 1, h], gr.at[far, d - 1, h], y_peer(d),
        )

    def gc(h):
        return remote(
            GKV.at[core, :, rows(h, HT)], GKV.at[core, :, rows(h, HT)],
            kvs.at[3 + h], kvr.at[3 + h], core_peer,
        )

    def tiles_send():
        for cp in kt_loads:
            cp.wait()
        KT[...] = jnp.transpose(KV[...])

    def tiles():
        pair_copy.wait_recv()
        lane = lax.broadcasted_iota(jnp.int32, (512, 128), 1)
        mine = (lane < 64) == (core == 0)
        GKV[core, chip] = jnp.where(mine, KT[...], pltpu.roll(KP[...], 64, 1))
        for h in range(2):
            gx(h).start()

    def gather_near(h):
        for d in (1, 3, 2):
            gy(d, h, 0).start()

    def gather_far(h):
        gx(h).wait_recv()
        for d in (1, 3, 2):
            gy(d, h, 1).start()

    def fwd_first(k):
        fwd_out(1, k).wait_recv()
        fwd_factor(1, k)
        fwd_back(1, k).start()

    def weights(part):
        for step in range(2 * part, 2 * part + 2):
            w_load(step).wait()
            s, base = step // 8, (step % 8) * 128

            def strip(i, carry, s=s, base=base, slot=step % 4):
                hi, lo = split(ST[slot, pl.ds(pl.multiple_of(i * 32, 32), 32), :])
                at = pl.ds(pl.multiple_of(base + i * 32, 32), 32)
                for q in range(4):
                    WH[s, q, at, :] = hi[:, q * 256 : (q + 1) * 256]
                    WL[s, q, at, :] = lo[:, q * 256 : (q + 1) * 256]
                return carry

            lax.fori_loop(0, 4, strip, 0)
            if step + 4 < 16:
                w_load(step + 4).start()

    x_again = [x_loads(k, lambda k, h: BS.at[2 * k + h // 4, h % 4], None, 1) for k in range(NC)]

    def gathered(h):
        for far in range(2):
            for d in (1, 3, 2):
                gy(d, h, far).wait_recv()
        gc(h).start()

    def upstream(h):
        gc(h).wait_recv()
        for s in range(2):
            for t in range(8):
                hi, lo = split(GKV[s, t, h * HT : (h + 1) * HT, :])
                col = (t % 4) * 2 + t // 4
                LH[s, :, col * 128 : (col + 1) * 128] = hi
                LL[s, :, col * 128 : (col + 1) * 128] = lo
        for u in range(2):

            def one(n, carry, u=u):
                at = pl.ds(pl.multiple_of(u * 512 + n * 256, 256), 256)
                acc = None
                for s in range(2):
                    for q in range(4):
                        lh = LH[s, :, q * 256 : (q + 1) * 256]
                        ll = LL[s, :, q * 256 : (q + 1) * 256]
                        part = dot3(lh, ll, WH[s, q, at, :], WL[s, q, at, :], 1, 1)
                        acc = part if acc is None else acc + part
                G[3, u, 2 * n, h * HT : (h + 1) * HT] = acc[:, :128]
                G[3, u, 2 * n + 1, h * HT : (h + 1) * HT] = acc[:, 128:]
                return carry

            lax.fori_loop(0, 2, one, 0)

    def fwd_step(m, k):
        fwd_out(m, k).wait_recv()
        fwd_factor(m, k)
        fwd_back(m, k).start()

    def bwd_step(m, k):
        bwd_out(m, k).wait_recv()
        bwd_factor(m, k)
        bwd_back(m, k).start()

    def fwd_next(m, k):
        fwd_back(m - 1, k).wait_recv()
        fwd_out(m, k).start()

    def bwd_next(m, k):
        bwd_back(m + 1, k).wait_recv()
        bwd_out(m, k).start()

    def gradient(m, t):
        own = 0 if m == 0 else bits[m]

        def one(c, carry):
            if m == 0:
                left = jnp.concatenate(
                    [
                        jnp.concatenate(
                            [BS[2 * k + lax.div(c, 2), 2 * lax.rem(c, 2) + i] for i in range(2)], axis=1
                        )
                        for k in (2 * t, 2 * t + 1)
                    ],
                    axis=0,
                )
                u, base = lax.div(c, 2), 2 * lax.rem(c, 2)
                right = jnp.concatenate([G[0, u, base + i, t * HT : (t + 1) * HT] for i in range(2)], axis=1)
            else:
                at = slice(t * HT, (t + 1) * HT)
                left = jnp.concatenate([R[m - 1, own, c, at], I[m - 1, c, at]], axis=1)
                right = jnp.concatenate([G[m, own, c, at], J[m - 1, c, at]], axis=1)
            lh, ll = split(left)
            rh, rl = split(right)
            total = dot3(lh, ll, rh, rl, 0, 0)
            table = TT[m]
            for i in range(2):
                hi, lo = split(total[i * 128 : (i + 1) * 128])
                back = jnp.dot(table, hi, preferred_element_type=F32) + jnp.dot(
                    table, lo, preferred_element_type=F32
                )
                ii = i if m == 0 else lax.rem(own + i, 2)
                for j in range(2):
                    jj = j if m == 0 else lax.rem(own + j, 2)
                    for zz in range(4):
                        piece = back[zz * 32 : (zz + 1) * 32, j * 128 : (j + 1) * 128]
                        GO[m, zz, ii, c, jj] = piece if t == 0 else GO[m, zz, ii, c, jj] + piece
            return carry

        lax.fori_loop(0, 4, one, 0)
        if t == 1 and m == 0:
            for zz in range(4):
                x_first(zz).start()
        if t == 1 and m > 0:
            for d in (1, 3, 2):
                z_send(m, d).start()

    def x_land(zz):
        return XG.at[0] if zz == 3 else GL.at[0, zz, 1]

    def x_first(zz):
        return remote(
            GO.at[0, zz, 1 - xlo], x_land(zz), zs.at[4, zz], zr.at[4, zz], xlo_peer
        )

    def z_last(d):
        return remote(
            GO.at[0, lax.rem(z + d, 4), xlo], GL.at[0, d - 1, 0], zs.at[0, d - 1], zr.at[0, d - 1], z_peer(d)
        )

    def x_sum(m):
        for zz in range(4):
            x_first(zz).wait_recv()
            GO[0, zz, xlo] = GO[0, zz, xlo] + x_land(zz)[...]
        for d in (1, 3, 2):
            z_last(d).start()

    def z_send(m, d):
        return remote(
            GO.at[m, lax.rem(z + d, 4)], GL.at[m, d - 1], zs.at[m, d - 1], zr.at[m, d - 1], z_peer(d)
        )

    def u_send(m):
        return remote(GO.at[m, z, 1 - xlo], XG.at[m], us.at[m], ur.at[m], xlo_peer)

    def z_sum(m):
        for d in (1, 3, 2):
            z_send(m, d).wait_recv()
        for side in (1 - xlo, xlo):
            GO[m, z, side] = GO[m, z, side] + GL[m, 0, side] + GL[m, 1, side] + GL[m, 2, side]
        u_send(m).start()

    def share_sum(m):
        if m == 0:
            for d in (1, 3, 2):
                z_last(d).wait_recv()
            GO[0, z, xlo] = GO[0, z, xlo] + GL[0, 0, 0] + GL[0, 1, 0] + GL[0, 2, 0]
        else:
            u_send(m).wait_recv()
            GO[m, z, xlo] = GO[m, z, xlo] + XG[m]
        result(m).start()

    def result(m):
        return local_copy(GO.at[m, z, xlo], go.at[m], osem.at[m])

    def kv_result(k):
        return local_copy(KV.at[:, rows(k)], kvo.at[:, rows(k)], osem.at[4 + k])

    def p_core(k):
        return remote(
            XP.at[k % 2, 1 - core], GKV.at[0, :, rows(k)], ps.at[0, k], pr.at[0, k], core_peer
        )

    def p_x(k):
        return remote(
            XP.at[k % 2, core, pl.ds(4 * (1 - xhi), 4)], XL.at[k], ps.at[4, k], pr.at[4, k], x_peer
        )

    def p_y(k, d):
        return remote(
            XP.at[k % 2, core, 4 * xhi + lax.rem(y + d, 4)], YL.at[d - 1, k], ps.at[d, k], pr.at[d, k], y_peer(d)
        )

    def p_all(k):
        found = []
        for slot, d, other in ((4, 1, 1), (6, 3, 1), (5, 2, 1), (3, 0, 1), (0, 1, 0), (2, 3, 0), (1, 2, 0)):
            side = 1 - xhi if other else xhi
            dev = (x_peer if d == 0 else xy_peer(d)) if other else y_peer(d)
            found.append(
                remote(
                    XP.at[k % 2, core, 4 * side + lax.rem(y + d, 4)], DL.at[slot, k - 2],
                    ps.at[6 + slot, k], pr.at[6 + slot, k], dev,
                )
            )
        return found

    def p_last(k):
        return remote(FT.at[k], KP.at[rows(k)], ps.at[5, k], pr.at[5, k], core_peer)

    def project(k):
        if k >= 2:
            p_core(k - 2).wait_send()
            for d in (1, 3, 2):
                p_y(k - 2, d).wait_send()
            p_x(k - 2).wait_send()
        for u in range(2):
            for c in range(4):
                hi, lo = split(R[3, u, c, k * CT : (k + 1) * CT])
                at = slice((u * 4 + c) * 128, (u * 4 + c + 1) * 128)
                LH[0, :CT, at] = hi
                LL[0, :CT, at] = lo
        for s in range(2):

            def one(n, carry, s=s):
                out = dot3(LH[0, :CT, :], LL[0, :CT, :], WH[s, n], WL[s, n])
                XP[k % 2, s, n] = out[:, :128]
                XP[k % 2, s, 4 + n] = out[:, 128:]
                return carry

            lax.fori_loop(0, 4, one, 0)
        p_core(k).start()

    def project_y(k):
        p_core(k).wait_recv()

        def one(t, carry):
            XP[k % 2, core, t] = XP[k % 2, core, t] + GKV[0, t, k * CT : (k + 1) * CT]
            return carry

        lax.fori_loop(0, 8, one, 0)
        if k < 2:
            p_x(k).start()
        else:
            for cp in p_all(k):
                cp.start()

    def project_x(k):
        p_x(k).wait_recv()
        for t in range(4):
            XP[k % 2, core, 4 * xhi + t] = XP[k % 2, core, 4 * xhi + t] + XL[k, t]
        for d in (1, 3, 2):
            p_y(k, d).start()

    def project_last(k):
        total = None
        if k < 2:
            for d in (1, 3, 2):
                p_y(k, d).wait_recv()
            total = XP[k % 2, core, chip] + YL[0, k] + YL[1, k] + YL[2, k]
        else:
            for cp in p_all(k):
                cp.wait_recv()
            total = XP[k % 2, core, chip]
            for slot in range(7):
                total = total + DL[slot, k - 2]
        FT[k] = total
        p_last(k).start()

    def project_out(k):
        p_last(k).wait_recv()
        at = slice(k * CT, (k + 1) * CT)
        key_tile = jnp.where(core == 0, FT[k], KP[at])
        value_tile = jnp.where(core == 0, KP[at], FT[k])
        key_tile = jnp.transpose(key_tile)
        value_tile = jnp.transpose(value_tile)
        KV[:64, at] = jnp.where(core == 0, key_tile[:64], key_tile[64:])
        KV[64:, at] = jnp.where(core == 0, value_tile[:64], value_tile[64:])
        kv_result(k).start()

    def fwd_last(k):
        bwd_back(3, k).wait_send()
        fwd_step(3, k)

    def bwd_mid(k):
        fwd_back(2, k).wait_send()
        bwd_step(2, k)

    def bwd_low(k):
        fwd_back(1, k).wait_send()
        bwd_step(1, k)

    def gather_done():
        for h in range(2):
            gx(h).wait_send()
            gc(h).wait_send()
            for far in range(2):
                for d in (1, 3, 2):
                    gy(d, h, far).wait_send()

    def bwd_low_out(k):
        if k == 0:
            gather_done()
        bwd_next(1, k)

    def bwd_grad0(t):
        for k in (2 * t, 2 * t + 1):
            bwd_back(1, k).wait_recv()
            for cp in x_again[k]:
                cp.wait()
        gradient(0, t)

    def project_in(k):
        fwd_back(3, k).wait_recv()
        project(k)

    def late_prepare(m):
        prepare(m, m % 2, third_blocks if m == 2 else fourth_blocks)
        if m == 3:
            for group in x_again:
                for cp in group:
                    cp.start()

    steps_of = {
        "Q": late_prepare,
        "T": tiles,
        "X": gather_far,
        "TY": gather_near,
        "Z": gathered,
        "W": weights,
        "H": upstream,
        "HS": lambda k: bwd_out(3, k).start(),
        "B": fwd_first,
        "C": lambda k: fwd_next(2, k),
        "D": lambda k: fwd_step(2, k),
        "E": lambda k: fwd_next(3, k),
        "F": fwd_last,
        "I": lambda k: bwd_step(3, k),
        "J": lambda k: bwd_next(2, k),
        "K": bwd_mid,
        "L": bwd_low_out,
        "M": bwd_low,
        "G": gradient,
        "N": bwd_grad0,
        "P": project_in,
        "PY": project_y,
        "PX": project_x,
        "PL": project_last,
        "PO": project_out,
        "S": z_sum,
        "SX": x_sum,
        "U": share_sum,
    }

    tiles_send()
    for k in range(NC):
        first_factor(k)
    prepare(1, 1, second_blocks)
    fourth_blocks = block_loads(3, 1)
    for cp in fourth_blocks:
        cp.start()
    pl.semaphore_wait(barrier, len(peers))
    pair_copy.start()
    for k in range(NC):
        fwd_out(1, k).start()

    for name, *args in ORDER:
        steps_of[name](*args)

    for m in (1, 2, 3):
        for k in range(NC):
            fwd_out(m, k).wait_send()
            bwd_out(m, k).wait_send()
    for k in range(NC):
        fwd_back(3, k).wait_send()
        bwd_back(2, k).wait_send()
        bwd_back(1, k).wait_send()
        p_last(k).wait_send()
    for k in (2, 3):
        p_core(k).wait_send()
        for cp in p_all(k):
            cp.wait_send()
    pair_copy.wait_send()
    for m in range(4):
        for d in (1, 3, 2):
            (z_send(m, d) if m else z_last(d)).wait_send()
        if m:
            u_send(m).wait_send()
        result(m).wait()
    for zz in range(4):
        x_first(zz).wait_send()
    for k in range(NC):
        kv_result(k).wait()


def finish(g, kv, mo, se, bl, ko, vo, nb, nm, ns, GV, KB, A, isem, jsem, osem):
    tok = lax.axis_index("tok")
    share = pl.ds(pl.multiple_of(tok * 32, 32), 32)
    copy = pltpu.make_async_copy

    def loads(m):
        return [
            copy(g.at[m], GV.at[m], isem.at[0, m]),
            copy(mo.at[m], A.at[0, m], isem.at[1, m]),
            copy(se.at[m], A.at[1, m], isem.at[2, m]),
            copy(bl.at[m, :, share, :], A.at[2, m], isem.at[3, m]),
        ]

    def stores(m):
        return [copy(A.at[i, m], out.at[m], osem.at[i, m]) for i, out in enumerate((nm, ns, nb))]

    kv_load = copy(kv, KB, jsem.at[0])
    kv_load.start()
    every = [loads(m) for m in range(4)]
    for group in every:
        for cp in group:
            cp.start()
    kv_load.wait()
    kv_stores = [
        copy(KB.at[pl.ds(0, 64)], ko, jsem.at[1]),
        copy(KB.at[pl.ds(64, 64)], vo, jsem.at[2]),
    ]
    for cp in kv_stores:
        cp.start()
    for m in range(4):
        for cp in every[m]:
            cp.wait()
        for c in range(4):
            for j in range(2):
                at = slice(j * 128, (j + 1) * 128)
                grad = GV[m, c, j]
                moment = beta_one * A[0, m, c, :, at] + (1.0 - beta_one) * grad
                second = beta_two * A[1, m, c, :, at] + (1.0 - beta_two) * grad * grad
                step = learn_rate * (moment / bias_one) / (jnp.sqrt(second / bias_two) + epsilon)
                A[0, m, c, :, at] = moment
                A[1, m, c, :, at] = second
                A[2, m, c, :, at] = A[2, m, c, :, at] - step
        for cp in stores(m):
            cp.start()
    for m in range(4):
        for cp in stores(m):
            cp.wait()
    for cp in kv_stores:
        cp.wait()


def local(x, kw, vw, bl, ro, kg, vg, mo, se):
    hbm = pl.BlockSpec(memory_space=pl.ANY)
    vmem = pl.BlockSpec(memory_space=pltpu.VMEM)
    dma = pltpu.SemaphoreType.DMA
    tile = (128, 128)
    scratch = [
        pltpu.VMEM((2, 2, 8) + tile, F32),
        pltpu.VMEM((2, 4, 1024, 256), BF16),
        pltpu.VMEM((2, 4, 1024, 256), BF16),
        pltpu.VMEM((4, 4, 256, 256), BF16),
        pltpu.VMEM((4, 4, 256, 256), BF16),
        pltpu.VMEM((4,) + tile, BF16),
        pltpu.VMEM((4,) + tile, BF16),
        pltpu.VMEM((4, 128, 1024), F32),
        pltpu.VMEM((8, 4) + tile, F32),
        pltpu.VMEM((4, 2, 4, 512, 128), F32),
        pltpu.VMEM((3, 4, 512, 128), F32),
        pltpu.VMEM((3, 4, 512, 128), F32),
        pltpu.VMEM((4, 2, 4, 512, 128), F32),
        pltpu.VMEM((3, 4, 512, 128), F32),
        pltpu.VMEM((2, 8, 512, 128), F32),
        pltpu.VMEM((512, 128), F32),
        pltpu.VMEM((512, 128), F32),
        pltpu.VMEM((2, 256, 1024), BF16),
        pltpu.VMEM((2, 256, 1024), BF16),
        pltpu.VMEM((3, 2) + tile, F32),
        pltpu.VMEM((2, 4) + tile, F32),
        pltpu.VMEM((7, 2) + tile, F32),
        pltpu.VMEM((4,) + tile, F32),
        pltpu.VMEM((4, 4, 2, 4, 2, 32, 128), F32),
        pltpu.VMEM((4, 3, 2, 4, 2, 32, 128), F32),
        pltpu.VMEM((4, 4, 2, 32, 128), F32),
        pltpu.VMEM((128, 512), F32),
        dma((4, 4)),
        dma((2, 4, 8)),
        dma((4,)),
        dma((2,)),
        dma((8,)),
        dma((2, 3, 2, 4)),
        dma((2, 3, 2, 4)),
        dma((5,)),
        dma((5,)),
        dma((2, 3, 2)),
        dma((2, 3, 2)),
        dma((13, 4)),
        dma((13, 4)),
        dma((5, 4)),
        dma((5, 4)),
        dma((4,)),
        dma((4,)),
    ]
    share = jax.ShapeDtypeStruct((4, 4, 32, 256), F32)
    narrow = jax.ShapeDtypeStruct((64, 512), F32)
    grads, kv = pl.pallas_call(
        kernel,
        out_shape=(
            jax.ShapeDtypeStruct((4, 4, 2, 32, 128), F32),
            jax.ShapeDtypeStruct((128, 512), F32),
        ),
        in_specs=[hbm, hbm, hbm, hbm, vmem, hbm, hbm],
        out_specs=(hbm, hbm),
        scratch_shapes=scratch,
        compiler_params=pltpu.CompilerParams(
            collective_id=0, has_side_effects=True, vmem_limit_bytes=67043328
        ),
    )(x, kw, vw, bl, ro, kg.T, vg.T)
    ko, vo, nb, nm, ns = pl.pallas_call(
        finish,
        out_shape=(narrow, narrow, share, share, share),
        in_specs=[hbm] * 5,
        out_specs=(hbm,) * 5,
        scratch_shapes=[
            pltpu.VMEM((4, 4, 2, 32, 128), F32),
            pltpu.VMEM((128, 512), F32),
            pltpu.VMEM((3, 4, 4, 32, 256), F32),
            dma((4, 4)),
            dma((3,)),
            dma((3, 4)),
        ],
    )(grads, kv, mo, se, bl)
    return ko.T, vo.T, nb, nm, ns


def solution(mesh):
    placed = (
        P("tok", "feat"),
        P("feat", None),
        P("feat", None),
        P(None, "feat", None, None),
        P(),
        P("tok", "feat"),
        P("tok", "feat"),
        P(None, "feat", "tok", None),
        P(None, "feat", "tok", None),
    )
    return jax.shard_map(
        local,
        mesh=mesh,
        in_specs=placed,
        out_specs=(
            P("tok", "feat"),
            P("tok", "feat"),
            P(None, "feat", "tok", None),
            P(None, "feat", "tok", None),
            P(None, "feat", "tok", None),
        ),
        check_vma=False,
    )
```

```python
import jax
import jax.numpy as jnp
from jax import lax
from jax.experimental import pallas as pl
from jax.experimental.pallas import tpu as pltpu
from jax.sharding import PartitionSpec as P

MESH = pl.DeviceIdType.MESH
F32 = jnp.float32
BF16 = jnp.bfloat16
beta_one = 0.9
beta_two = 0.95
learn_rate = 0.01
epsilon = 1e-08
bias_one = 1.0 - 0.9**10
bias_two = 1.0 - 0.95**10

ORDER = (
    ("T",), ("Q", 1), ("W", 0), ("TY", 0), ("B", 3), ("B", 1), ("C", 3), ("B", 0), ("W", 1),
    ("X", 0), ("W", 2), ("X", 1), ("Q", 2), ("B", 2), ("W", 3), ("C", 0), ("C", 1), ("C", 2),
    ("TY", 1), ("W", 4), ("D", 3), ("W", 5), ("W", 6), ("Z", 0), ("W", 7), ("H", 0), ("HS", 0),
    ("Q", 3), ("D", 0), ("Z", 1), ("HS", 1), ("D", 1), ("I", 0), ("H", 1), ("I", 1), ("J", 0),
    ("HS", 3), ("J", 1), ("HS", 2), ("K", 0), ("I", 3), ("K", 1), ("I", 2), ("G", 2, 0), ("E", 1),
    ("E", 0), ("L", 0), ("J", 3), ("M", 0), ("L", 1), ("J", 2), ("M", 1), ("G", 1, 0), ("K", 3),
    ("F", 1), ("D", 2), ("N", 0), ("K", 2), ("F", 0), ("G", 2, 1), ("E", 3), ("L", 3), ("P", 1),
    ("M", 3), ("E", 2), ("PY", 1), ("P", 0), ("L", 2), ("PY", 0), ("F", 3), ("M", 2), ("S", 2),
    ("G", 1, 1), ("PX", 1), ("N", 1), ("F", 2), ("G", 3, 0), ("PX", 0), ("G", 3, 1), ("U", 2),
    ("PL", 1), ("P", 3), ("PY", 3), ("S", 1), ("PL", 0), ("P", 2), ("SX", 0), ("PO", 1), ("PY", 2),
    ("PL", 3), ("S", 3), ("U", 1), ("PO", 0), ("PO", 3), ("U", 0), ("PL", 2), ("PO", 2), ("U", 3),
)

CT = 128
NC = 4
HT = 256


def split(v):
    hi = v.astype(BF16)
    lo = (v - hi.astype(F32)).astype(BF16)
    return hi, lo


def dims(ca, cb):
    return (((ca,), (cb,)), ((), ()))


def dot3(ah, al, bh, bl, ca=1, cb=0):
    d = dims(ca, cb)
    out = lax.dot_general(ah, bh, d, preferred_element_type=F32)
    out = out + lax.dot_general(ah, bl, d, preferred_element_type=F32)
    return out + lax.dot_general(al, bh, d, preferred_element_type=F32)


def kernel(
    x, kw, vw, bl, ro, kg, vg,
    go, kvo,
    XP, WH, WL, AH, AL, TT, TS, ST, BS, R, I, T, G, J, GKV, KT, KP, LH, LL, YL, XL, DL, FT, GO, GL, XG, KV,
    bsem, xsem, stsem, ktsem, osem,
    ss, rs, kvs, kvr, gs, gr, ps, pr, zs, zr, us, ur,
):
    tok = lax.axis_index("tok")
    feat = lax.axis_index("feat")
    z = lax.rem(tok, 4)
    xlo = lax.div(tok, 4)
    core = lax.rem(feat, 2)
    xhi = lax.rem(lax.div(feat, 2), 2)
    y = lax.div(feat, 4)
    yhi = lax.div(feat, 8)
    yx = lax.rem(feat, 4)
    chip = xhi * 4 + y
    bits = [None, core, xhi, yhi]
    steps = [None, 1, 2, 8]

    def flip(m):
        return (tok, feat + steps[m] - 2 * steps[m] * bits[m])

    core_peer, x_peer = flip(1), flip(2)

    def y_peer(d):
        return (tok, lax.rem(y + d, 4) * 4 + yx)

    def xy_peer(d):
        return (tok, lax.rem(y + d, 4) * 4 + yx + 2 - 4 * xhi)

    def z_peer(d):
        return (xlo * 4 + lax.rem(z + d, 4), feat)

    xlo_peer = (lax.rem(tok + 4, 8), feat)

    def local_copy(src, dst, sem):
        return pltpu.make_async_copy(src, dst, sem)

    def remote(src, dst, s, r, dev):
        return pltpu.make_async_remote_copy(
            src_ref=src, dst_ref=dst, send_sem=s, recv_sem=r, device_id=dev, device_id_type=MESH
        )

    def rows(k, n=CT):
        return pl.ds(pl.multiple_of(k * n, n), n)

    def block_loads(m, slot):
        copies = []
        for i in range(2):
            for j in range(2):
                if m == 0:
                    r0, c0 = i * 128, j * 128
                else:
                    r0 = pl.multiple_of(lax.rem(bits[m] + i, 2) * 128, 128)
                    c0 = pl.multiple_of(lax.rem(bits[m] + j, 2) * 128, 128)
                copies.append(
                    local_copy(
                        bl.at[m, :, pl.ds(r0, 128), pl.ds(c0, 128)],
                        BS.at[pl.ds(4 * slot, 4), 2 * i + j],
                        bsem.at[m, 2 * i + j],
                    )
                )
        return copies

    def x_loads(k, to, at, sem):
        return [
            local_copy(x.at[pl.ds(k * CT, CT), pl.ds(h * 128, 128)], to(k, h), xsem.at[sem, k, h])
            for h in range(8)
        ]

    kt_loads = [
        local_copy(kg, KV.at[pl.ds(0, 64)], ktsem.at[0]),
        local_copy(vg, KV.at[pl.ds(64, 64)], ktsem.at[1]),
    ]
    for cp in kt_loads:
        cp.start()
    first_blocks = block_loads(0, 0)
    for cp in first_blocks:
        cp.start()
    x_copies = [x_loads(k, lambda k, h: XP.at[k // 2, k % 2, h], None, 0) for k in range(NC)]
    for cp in x_copies[0]:
        cp.start()
    second_blocks = block_loads(1, 1)
    for cp in second_blocks:
        cp.start()
    for k in range(1, NC):
        for cp in x_copies[k]:
            cp.start()

    def w_load(step):
        src = kw if step < 8 else vw
        return local_copy(src.at[pl.ds((step % 8) * 128, 128), :], ST.at[step % 4], stsem.at[step % 4])

    for step in range(4):
        w_load(step).start()

    barrier = pltpu.get_barrier_semaphore()
    peers = [core_peer, x_peer, y_peer(1), y_peer(2), y_peer(3), z_peer(1), z_peer(2), z_peer(3), xlo_peer]
    peers += [xy_peer(1), xy_peer(2), xy_peer(3)]
    for dev in peers:
        pl.semaphore_signal(barrier, inc=1, device_id=dev, device_id_type=MESH)

    for m in range(4):
        order = jnp.broadcast_to(ro[m : m + 1, :], (128, 128))
        hot = (lax.broadcasted_iota(jnp.int32, (128, 128), 0) == order).astype(F32)
        TT[m] = hot.astype(BF16)
        TS[m] = jnp.transpose(hot).astype(BF16)

    def prepare(m, slot, copies):
        for cp in copies:
            cp.wait()
        table = TS[m]

        def one(c, carry):
            for i in range(2):
                for j in range(2):
                    hi, lo = split(BS[4 * slot + c, 2 * i + j])
                    ph = jnp.dot(table, hi, preferred_element_type=F32)
                    p_lo = jnp.dot(table, lo, preferred_element_type=F32)
                    AH[m, c, i * 128 : (i + 1) * 128, j * 128 : (j + 1) * 128] = ph.astype(BF16)
                    AL[m, c, i * 128 : (i + 1) * 128, j * 128 : (j + 1) * 128] = p_lo.astype(BF16)
            return carry

        lax.fori_loop(0, 4, one, 0)

    def fwd_out(m, k):
        return remote(
            R.at[m - 1, 1 - bits[m], :, rows(k)], I.at[m - 1, :, rows(k)],
            ss.at[0, m - 1, 0, k], rs.at[0, m - 1, 0, k], flip(m),
        )

    def fwd_back(m, k):
        return remote(
            T.at[m - 1, :, rows(k)], R.at[m, bits[m], :, rows(k)],
            ss.at[0, m - 1, 1, k], rs.at[0, m - 1, 1, k], flip(m),
        )

    def bwd_out(m, k):
        return remote(
            G.at[m, 1 - bits[m], :, rows(k)], J.at[m - 1, :, rows(k)],
            ss.at[1, m - 1, 0, k], rs.at[1, m - 1, 0, k], flip(m),
        )

    def bwd_back(m, k):
        return remote(
            T.at[3 if m == 2 else m - 1, :, rows(k)], G.at[m - 1, bits[m], :, rows(k)],
            ss.at[1, m - 1, 1, k], rs.at[1, m - 1, 1, k], flip(m),
        )

    def first_factor(k):
        for cp in x_copies[k]:
            cp.wait()
        for u in range(2):
            for c in range(2):
                h = 4 * u + 2 * c
                pair = jnp.concatenate([XP[k // 2, k % 2, h], XP[k // 2, k % 2, h + 1]], axis=1)
                hi, lo = split(pair)
                out = dot3(hi, lo, AH[0, 2 * u + c], AL[0, 2 * u + c])
                R[0, u, 2 * c, k * CT : (k + 1) * CT] = out[:, :128]
                R[0, u, 2 * c + 1, k * CT : (k + 1) * CT] = out[:, 128:]

    def fwd_factor(m, k):
        own = bits[m]

        def one(c, carry):
            pair = jnp.concatenate([R[m - 1, own, c, rows(k)], I[m - 1, c, rows(k)]], axis=1)
            hi, lo = split(pair)
            out = dot3(hi, lo, AH[m, c], AL[m, c])
            R[m, own, c, rows(k)] = out[:, :128]
            T[m - 1, c, rows(k)] = out[:, 128:]
            return carry

        lax.fori_loop(0, 4, one, 0)

    def bwd_factor(m, k):
        own = bits[m]

        def one(c, carry):
            pair = jnp.concatenate([G[m, own, c, rows(k)], J[m - 1, c, rows(k)]], axis=1)
            hi, lo = split(pair)
            out = dot3(hi, lo, AH[m, c], AL[m, c], 1, 1)
            G[m - 1, own, c, rows(k)] = out[:, :128]
            T[3 if m == 2 else m - 1, c, rows(k)] = out[:, 128:]
            return carry

        lax.fori_loop(0, 4, one, 0)

    pair_copy = remote(KT, KP, kvs.at[0], kvr.at[0], core_peer)
    chip_x = (1 - xhi) * 4 + y

    def gx(h):
        return remote(
            GKV.at[core, chip, rows(h, HT)], GKV.at[core, chip, rows(h, HT)],
            kvs.at[1 + h], kvr.at[1 + h], x_peer,
        )

    def gy(d, h, far):
        tile = chip_x if far else chip
        return remote(
            GKV.at[core, tile, rows(h, HT)], GKV.at[core, tile, rows(h, HT)],
            gs.at[far, d - 1, h], gr.at[far, d - 1, h], y_peer(d),
        )

    def gc(h):
        return remote(
            GKV.at[core, :, rows(h, HT)], GKV.at[core, :, rows(h, HT)],
            kvs.at[3 + h], kvr.at[3 + h], core_peer,
        )

    def tiles_send():
        for cp in kt_loads:
            cp.wait()
        KT[...] = jnp.transpose(KV[...])

    def tiles():
        pair_copy.wait_recv()
        lane = lax.broadcasted_iota(jnp.int32, (512, 128), 1)
        mine = (lane < 64) == (core == 0)
        GKV[core, chip] = jnp.where(mine, KT[...], pltpu.roll(KP[...], 64, 1))
        for h in range(2):
            gx(h).start()

    def gather_near(h):
        for d in (1, 3, 2):
            gy(d, h, 0).start()

    def gather_far(h):
        gx(h).wait_recv()
        for d in (1, 3, 2):
            gy(d, h, 1).start()

    def fwd_first(k):
        fwd_out(1, k).wait_recv()
        fwd_factor(1, k)
        fwd_back(1, k).start()

    def weights(part):
        for step in range(2 * part, 2 * part + 2):
            w_load(step).wait()
            s, base = step // 8, (step % 8) * 128

            def strip(i, carry, s=s, base=base, slot=step % 4):
                hi, lo = split(ST[slot, pl.ds(pl.multiple_of(i * 32, 32), 32), :])
                at = pl.ds(pl.multiple_of(base + i * 32, 32), 32)
                for q in range(4):
                    WH[s, q, at, :] = hi[:, q * 256 : (q + 1) * 256]
                    WL[s, q, at, :] = lo[:, q * 256 : (q + 1) * 256]
                return carry

            lax.fori_loop(0, 4, strip, 0)
            if step + 4 < 16:
                w_load(step + 4).start()

    x_again = [x_loads(k, lambda k, h: BS.at[2 * k + h // 4, h % 4], None, 1) for k in range(NC)]

    def gathered(h):
        for far in range(2):
            for d in (1, 3, 2):
                gy(d, h, far).wait_recv()
        gc(h).start()

    def upstream(h):
        gc(h).wait_recv()
        for s in range(2):
            for t in range(8):
                hi, lo = split(GKV[s, t, h * HT : (h + 1) * HT, :])
                col = (t % 4) * 2 + t // 4
                LH[s, :, col * 128 : (col + 1) * 128] = hi
                LL[s, :, col * 128 : (col + 1) * 128] = lo
        for u in range(2):

            def one(n, carry, u=u):
                at = pl.ds(pl.multiple_of(u * 512 + n * 256, 256), 256)
                acc = None
                for s in range(2):
                    for q in range(4):
                        lh = LH[s, :, q * 256 : (q + 1) * 256]
                        ll = LL[s, :, q * 256 : (q + 1) * 256]
                        part = dot3(lh, ll, WH[s, q, at, :], WL[s, q, at, :], 1, 1)
                        acc = part if acc is None else acc + part
                G[3, u, 2 * n, h * HT : (h + 1) * HT] = acc[:, :128]
                G[3, u, 2 * n + 1, h * HT : (h + 1) * HT] = acc[:, 128:]
                return carry

            lax.fori_loop(0, 2, one, 0)

    def fwd_step(m, k):
        fwd_out(m, k).wait_recv()
        fwd_factor(m, k)
        fwd_back(m, k).start()

    def bwd_step(m, k):
        bwd_out(m, k).wait_recv()
        bwd_factor(m, k)
        bwd_back(m, k).start()

    def fwd_next(m, k):
        fwd_back(m - 1, k).wait_recv()
        fwd_out(m, k).start()

    def bwd_next(m, k):
        bwd_back(m + 1, k).wait_recv()
        bwd_out(m, k).start()

    def gradient(m, t):
        own = 0 if m == 0 else bits[m]

        def one(c, carry):
            if m == 0:
                left = jnp.concatenate(
                    [
                        jnp.concatenate(
                            [BS[2 * k + lax.div(c, 2), 2 * lax.rem(c, 2) + i] for i in range(2)], axis=1
                        )
                        for k in (2 * t, 2 * t + 1)
                    ],
                    axis=0,
                )
                u, base = lax.div(c, 2), 2 * lax.rem(c, 2)
                right = jnp.concatenate([G[0, u, base + i, t * HT : (t + 1) * HT] for i in range(2)], axis=1)
            else:
                at = slice(t * HT, (t + 1) * HT)
                left = jnp.concatenate([R[m - 1, own, c, at], I[m - 1, c, at]], axis=1)
                right = jnp.concatenate([G[m, own, c, at], J[m - 1, c, at]], axis=1)
            lh, ll = split(left)
            rh, rl = split(right)
            total = dot3(lh, ll, rh, rl, 0, 0)
            table = TT[m]
            for i in range(2):
                hi, lo = split(total[i * 128 : (i + 1) * 128])
                back = jnp.dot(table, hi, preferred_element_type=F32) + jnp.dot(
                    table, lo, preferred_element_type=F32
                )
                ii = i if m == 0 else lax.rem(own + i, 2)
                for j in range(2):
                    jj = j if m == 0 else lax.rem(own + j, 2)
                    for zz in range(4):
                        piece = back[zz * 32 : (zz + 1) * 32, j * 128 : (j + 1) * 128]
                        GO[m, zz, ii, c, jj] = piece if t == 0 else GO[m, zz, ii, c, jj] + piece
            return carry

        lax.fori_loop(0, 4, one, 0)
        if t == 1 and m == 0:
            for zz in range(4):
                x_first(zz).start()
        if t == 1 and m > 0:
            for d in (1, 3, 2):
                z_send(m, d).start()

    def x_land(zz):
        return XG.at[0] if zz == 3 else GL.at[0, zz, 1]

    def x_first(zz):
        return remote(
            GO.at[0, zz, 1 - xlo], x_land(zz), zs.at[4, zz], zr.at[4, zz], xlo_peer
        )

    def z_last(d):
        return remote(
            GO.at[0, lax.rem(z + d, 4), xlo], GL.at[0, d - 1, 0], zs.at[0, d - 1], zr.at[0, d - 1], z_peer(d)
        )

    def x_sum(m):
        for zz in range(4):
            x_first(zz).wait_recv()
            GO[0, zz, xlo] = GO[0, zz, xlo] + x_land(zz)[...]
        for d in (1, 3, 2):
            z_last(d).start()

    def z_send(m, d):
        return remote(
            GO.at[m, lax.rem(z + d, 4)], GL.at[m, d - 1], zs.at[m, d - 1], zr.at[m, d - 1], z_peer(d)
        )

    def u_send(m):
        return remote(GO.at[m, z, 1 - xlo], XG.at[m], us.at[m], ur.at[m], xlo_peer)

    def z_sum(m):
        for d in (1, 3, 2):
            z_send(m, d).wait_recv()
        for side in (1 - xlo, xlo):
            GO[m, z, side] = GO[m, z, side] + GL[m, 0, side] + GL[m, 1, side] + GL[m, 2, side]
        u_send(m).start()

    def share_sum(m):
        if m == 0:
            for d in (1, 3, 2):
                z_last(d).wait_recv()
            GO[0, z, xlo] = GO[0, z, xlo] + GL[0, 0, 0] + GL[0, 1, 0] + GL[0, 2, 0]
        else:
            u_send(m).wait_recv()
            GO[m, z, xlo] = GO[m, z, xlo] + XG[m]
        result(m).start()

    def result(m):
        return local_copy(GO.at[m, z, xlo], go.at[m], osem.at[m])

    def kv_result(k):
        return local_copy(KV.at[:, rows(k)], kvo.at[:, rows(k)], osem.at[4 + k])

    def p_core(k):
        return remote(
            XP.at[k % 2, 1 - core], GKV.at[0, :, rows(k)], ps.at[0, k], pr.at[0, k], core_peer
        )

    def p_x(k):
        return remote(
            XP.at[k % 2, core, pl.ds(4 * (1 - xhi), 4)], XL.at[k], ps.at[4, k], pr.at[4, k], x_peer
        )

    def p_y(k, d):
        return remote(
            XP.at[k % 2, core, 4 * xhi + lax.rem(y + d, 4)], YL.at[d - 1, k], ps.at[d, k], pr.at[d, k], y_peer(d)
        )

    def p_all(k):
        found = []
        for slot, d, other in ((4, 1, 1), (6, 3, 1), (5, 2, 1), (3, 0, 1), (0, 1, 0), (2, 3, 0), (1, 2, 0)):
            side = 1 - xhi if other else xhi
            dev = (x_peer if d == 0 else xy_peer(d)) if other else y_peer(d)
            found.append(
                remote(
                    XP.at[k % 2, core, 4 * side + lax.rem(y + d, 4)], DL.at[slot, k - 2],
                    ps.at[6 + slot, k], pr.at[6 + slot, k], dev,
                )
            )
        return found

    def p_last(k):
        return remote(FT.at[k], KP.at[rows(k)], ps.at[5, k], pr.at[5, k], core_peer)

    def project(k):
        if k >= 2:
            p_core(k - 2).wait_send()
            for d in (1, 3, 2):
                p_y(k - 2, d).wait_send()
            p_x(k - 2).wait_send()
        for u in range(2):
            for c in range(4):
                hi, lo = split(R[3, u, c, k * CT : (k + 1) * CT])
                at = slice((u * 4 + c) * 128, (u * 4 + c + 1) * 128)
                LH[0, :CT, at] = hi
                LL[0, :CT, at] = lo
        for s in range(2):

            def one(n, carry, s=s):
                out = dot3(LH[0, :CT, :], LL[0, :CT, :], WH[s, n], WL[s, n])
                XP[k % 2, s, n] = out[:, :128]
                XP[k % 2, s, 4 + n] = out[:, 128:]
                return carry

            lax.fori_loop(0, 4, one, 0)
        p_core(k).start()

    def project_y(k):
        p_core(k).wait_recv()

        def one(t, carry):
            XP[k % 2, core, t] = XP[k % 2, core, t] + GKV[0, t, k * CT : (k + 1) * CT]
            return carry

        lax.fori_loop(0, 8, one, 0)
        if k < 2:
            p_x(k).start()
        else:
            for cp in p_all(k):
                cp.start()

    def project_x(k):
        p_x(k).wait_recv()
        for t in range(4):
            XP[k % 2, core, 4 * xhi + t] = XP[k % 2, core, 4 * xhi + t] + XL[k, t]
        for d in (1, 3, 2):
            p_y(k, d).start()

    def project_last(k):
        total = None
        if k < 2:
            for d in (1, 3, 2):
                p_y(k, d).wait_recv()
            total = XP[k % 2, core, chip] + YL[0, k] + YL[1, k] + YL[2, k]
        else:
            for cp in p_all(k):
                cp.wait_recv()
            total = XP[k % 2, core, chip]
            for slot in range(7):
                total = total + DL[slot, k - 2]
        FT[k] = total
        p_last(k).start()

    def project_out(k):
        p_last(k).wait_recv()
        at = slice(k * CT, (k + 1) * CT)
        key_tile = jnp.where(core == 0, FT[k], KP[at])
        value_tile = jnp.where(core == 0, KP[at], FT[k])
        key_tile = jnp.transpose(key_tile)
        value_tile = jnp.transpose(value_tile)
        KV[:64, at] = jnp.where(core == 0, key_tile[:64], key_tile[64:])
        KV[64:, at] = jnp.where(core == 0, value_tile[:64], value_tile[64:])
        kv_result(k).start()

    def fwd_last(k):
        bwd_back(3, k).wait_send()
        fwd_step(3, k)

    def bwd_mid(k):
        bwd_step(2, k)

    def bwd_low(k):
        fwd_back(1, k).wait_send()
        bwd_step(1, k)

    def gather_done():
        for h in range(2):
            gx(h).wait_send()
            gc(h).wait_send()
            for far in range(2):
                for d in (1, 3, 2):
                    gy(d, h, far).wait_send()

    def bwd_low_out(k):
        if k == 0:
            gather_done()
        bwd_next(1, k)

    def bwd_grad0(t):
        for k in (2 * t, 2 * t + 1):
            bwd_back(1, k).wait_recv()
            for cp in x_again[k]:
                cp.wait()
        gradient(0, t)

    def project_in(k):
        fwd_back(3, k).wait_recv()
        project(k)

    def late_prepare(m):
        prepare(m, m % 2, {1: second_blocks, 2: third_blocks, 3: fourth_blocks}[m])
        if m == 1:
            for cp in fourth_blocks:
                cp.start()
        if m == 3:
            for group in x_again:
                for cp in group:
                    cp.start()

    steps_of = {
        "Q": late_prepare,
        "T": tiles,
        "X": gather_far,
        "TY": gather_near,
        "Z": gathered,
        "W": weights,
        "H": upstream,
        "HS": lambda k: bwd_out(3, k).start(),
        "B": fwd_first,
        "C": lambda k: fwd_next(2, k),
        "D": lambda k: fwd_step(2, k),
        "E": lambda k: fwd_next(3, k),
        "F": fwd_last,
        "I": lambda k: bwd_step(3, k),
        "J": lambda k: bwd_next(2, k),
        "K": bwd_mid,
        "L": bwd_low_out,
        "M": bwd_low,
        "G": gradient,
        "N": bwd_grad0,
        "P": project_in,
        "PY": project_y,
        "PX": project_x,
        "PL": project_last,
        "PO": project_out,
        "S": z_sum,
        "SX": x_sum,
        "U": share_sum,
    }

    tiles_send()
    prepare(0, 0, first_blocks)
    third_blocks = block_loads(2, 0)
    for cp in third_blocks:
        cp.start()
    fourth_blocks = block_loads(3, 1)
    pl.semaphore_wait(barrier, len(peers))
    pair_copy.start()
    for k in range(NC):
        first_factor(k)
        fwd_out(1, k).start()

    for name, *args in ORDER:
        steps_of[name](*args)

    for m in (1, 2, 3):
        for k in range(NC):
            fwd_out(m, k).wait_send()
            bwd_out(m, k).wait_send()
    for k in range(NC):
        fwd_back(3, k).wait_send()
        fwd_back(2, k).wait_send()
        bwd_back(2, k).wait_send()
        bwd_back(1, k).wait_send()
        p_last(k).wait_send()
    for k in (2, 3):
        p_core(k).wait_send()
        for cp in p_all(k):
            cp.wait_send()
    pair_copy.wait_send()
    for m in range(4):
        for d in (1, 3, 2):
            (z_send(m, d) if m else z_last(d)).wait_send()
        if m:
            u_send(m).wait_send()
        result(m).wait()
    for zz in range(4):
        x_first(zz).wait_send()
    for k in range(NC):
        kv_result(k).wait()


def finish(g, kv, mo, se, bl, ko, vo, nb, nm, ns, GV, KB, A, isem, jsem, osem):
    tok = lax.axis_index("tok")
    share = pl.ds(pl.multiple_of(tok * 32, 32), 32)
    copy = pltpu.make_async_copy

    def loads(m):
        return [
            copy(g.at[m], GV.at[m], isem.at[0, m]),
            copy(mo.at[m], A.at[0, m], isem.at[1, m]),
            copy(se.at[m], A.at[1, m], isem.at[2, m]),
            copy(bl.at[m, :, share, :], A.at[2, m], isem.at[3, m]),
        ]

    def stores(m):
        return [copy(A.at[i, m], out.at[m], osem.at[i, m]) for i, out in enumerate((nm, ns, nb))]

    kv_load = copy(kv, KB, jsem.at[0])
    kv_load.start()
    every = [loads(m) for m in range(4)]
    for group in every:
        for cp in group:
            cp.start()
    kv_load.wait()
    kv_stores = [
        copy(KB.at[pl.ds(0, 64)], ko, jsem.at[1]),
        copy(KB.at[pl.ds(64, 64)], vo, jsem.at[2]),
    ]
    for cp in kv_stores:
        cp.start()
    for m in range(4):
        for cp in every[m]:
            cp.wait()
        for c in range(4):
            for j in range(2):
                at = slice(j * 128, (j + 1) * 128)
                grad = GV[m, c, j]
                moment = beta_one * A[0, m, c, :, at] + (1.0 - beta_one) * grad
                second = beta_two * A[1, m, c, :, at] + (1.0 - beta_two) * grad * grad
                step = learn_rate * (moment / bias_one) / (jnp.sqrt(second / bias_two) + epsilon)
                A[0, m, c, :, at] = moment
                A[1, m, c, :, at] = second
                A[2, m, c, :, at] = A[2, m, c, :, at] - step
        for cp in stores(m):
            cp.start()
    for m in range(4):
        for cp in stores(m):
            cp.wait()
    for cp in kv_stores:
        cp.wait()


def local(x, kw, vw, bl, ro, kg, vg, mo, se):
    hbm = pl.BlockSpec(memory_space=pl.ANY)
    vmem = pl.BlockSpec(memory_space=pltpu.VMEM)
    dma = pltpu.SemaphoreType.DMA
    tile = (128, 128)
    scratch = [
        pltpu.VMEM((2, 2, 8) + tile, F32),
        pltpu.VMEM((2, 4, 1024, 256), BF16),
        pltpu.VMEM((2, 4, 1024, 256), BF16),
        pltpu.VMEM((4, 4, 256, 256), BF16),
        pltpu.VMEM((4, 4, 256, 256), BF16),
        pltpu.VMEM((4,) + tile, BF16),
        pltpu.VMEM((4,) + tile, BF16),
        pltpu.VMEM((4, 128, 1024), F32),
        pltpu.VMEM((8, 4) + tile, F32),
        pltpu.VMEM((4, 2, 4, 512, 128), F32),
        pltpu.VMEM((3, 4, 512, 128), F32),
        pltpu.VMEM((4, 4, 512, 128), F32),
        pltpu.VMEM((4, 2, 4, 512, 128), F32),
        pltpu.VMEM((3, 4, 512, 128), F32),
        pltpu.VMEM((2, 8, 512, 128), F32),
        pltpu.VMEM((512, 128), F32),
        pltpu.VMEM((512, 128), F32),
        pltpu.VMEM((2, 256, 1024), BF16),
        pltpu.VMEM((2, 256, 1024), BF16),
        pltpu.VMEM((3, 2) + tile, F32),
        pltpu.VMEM((2, 4) + tile, F32),
        pltpu.VMEM((7, 2) + tile, F32),
        pltpu.VMEM((4,) + tile, F32),
        pltpu.VMEM((4, 4, 2, 4, 2, 32, 128), F32),
        pltpu.VMEM((4, 3, 2, 4, 2, 32, 128), F32),
        pltpu.VMEM((4, 4, 2, 32, 128), F32),
        pltpu.VMEM((128, 512), F32),
        dma((4, 4)),
        dma((2, 4, 8)),
        dma((4,)),
        dma((2,)),
        dma((8,)),
        dma((2, 3, 2, 4)),
        dma((2, 3, 2, 4)),
        dma((5,)),
        dma((5,)),
        dma((2, 3, 2)),
        dma((2, 3, 2)),
        dma((13, 4)),
        dma((13, 4)),
        dma((5, 4)),
        dma((5, 4)),
        dma((4,)),
        dma((4,)),
    ]
    share = jax.ShapeDtypeStruct((4, 4, 32, 256), F32)
    narrow = jax.ShapeDtypeStruct((64, 512), F32)
    grads, kv = pl.pallas_call(
        kernel,
        out_shape=(
            jax.ShapeDtypeStruct((4, 4, 2, 32, 128), F32),
            jax.ShapeDtypeStruct((128, 512), F32),
        ),
        in_specs=[hbm, hbm, hbm, hbm, vmem, hbm, hbm],
        out_specs=(hbm, hbm),
        scratch_shapes=scratch,
        compiler_params=pltpu.CompilerParams(
            collective_id=0, has_side_effects=True, vmem_limit_bytes=67043328
        ),
    )(x, kw, vw, bl, ro, kg.T, vg.T)
    ko, vo, nb, nm, ns = pl.pallas_call(
        finish,
        out_shape=(narrow, narrow, share, share, share),
        in_specs=[hbm] * 5,
        out_specs=(hbm,) * 5,
        scratch_shapes=[
            pltpu.VMEM((4, 4, 2, 32, 128), F32),
            pltpu.VMEM((128, 512), F32),
            pltpu.VMEM((3, 4, 4, 32, 256), F32),
            dma((4, 4)),
            dma((3,)),
            dma((3, 4)),
        ],
    )(grads, kv, mo, se, bl)
    return ko.T, vo.T, nb, nm, ns


def solution(mesh):
    placed = (
        P("tok", "feat"),
        P("feat", None),
        P("feat", None),
        P(None, "feat", None, None),
        P(),
        P("tok", "feat"),
        P("tok", "feat"),
        P(None, "feat", "tok", None),
        P(None, "feat", "tok", None),
    )
    return jax.shard_map(
        local,
        mesh=mesh,
        in_specs=placed,
        out_specs=(
            P("tok", "feat"),
            P("tok", "feat"),
            P(None, "feat", "tok", None),
            P(None, "feat", "tok", None),
            P(None, "feat", "tok", None),
        ),
        check_vma=False,
    )
```

```python
import jax
import jax.numpy as jnp
from jax import lax
from jax.experimental import pallas as pl
from jax.experimental.pallas import tpu as pltpu
from jax.sharding import PartitionSpec as P

MESH = pl.DeviceIdType.MESH
F32 = jnp.float32
BF16 = jnp.bfloat16
beta_one = 0.9
beta_two = 0.95
learn_rate = 0.01
epsilon = 1e-08
bias_one = 1.0 - 0.9**10
bias_two = 1.0 - 0.95**10

ORDER = (
    ("W", 0), ("W", 1), ("T",), ("TY", 0), ("B", 2), ("W", 2), ("Q", 2), ("W", 3), ("B", 0),
    ("C", 2), ("X", 0), ("Q", 3), ("TY", 1), ("C", 0), ("B", 1), ("B", 3), ("W", 4), ("W", 5),
    ("Z", 0), ("C", 3), ("C", 1), ("X", 1), ("W", 6), ("W", 7), ("H", 0), ("HS", 0), ("D", 0),
    ("HS", 1), ("D", 1), ("Z", 1), ("I", 0), ("D", 3), ("I", 1), ("H", 1), ("HS", 3), ("HS", 2),
    ("J", 0), ("J", 1), ("K", 0), ("I", 3), ("K", 1), ("I", 2), ("L", 0), ("J", 3), ("M", 0),
    ("E", 1), ("G", 2, 0), ("E", 0), ("L", 1), ("J", 2), ("M", 1), ("G", 1, 0), ("K", 3), ("F", 1),
    ("N", 0), ("D", 2), ("K", 2), ("F", 0), ("G", 2, 1), ("G", 3, 0), ("L", 3), ("E", 3), ("P", 1),
    ("M", 3), ("PY", 1), ("E", 2), ("P", 0), ("L", 2), ("PY", 0), ("F", 3), ("M", 2), ("S", 2),
    ("G", 1, 1), ("PX", 1), ("F", 2), ("N", 1), ("PX", 0), ("G", 3, 1), ("U", 2), ("PL", 1),
    ("P", 3), ("PY", 3), ("S", 1), ("PL", 0), ("P", 2), ("SX", 0), ("PY", 2), ("S", 3), ("U", 1),
    ("PL", 3), ("U", 0), ("PL", 2), ("PO", 2), ("PO", 3), ("PO", 0), ("PO", 1), ("U", 3),
)

CT = 128
NC = 4
HT = 256


def split(v):
    hi = v.astype(BF16)
    lo = (v - hi.astype(F32)).astype(BF16)
    return hi, lo


def dims(ca, cb):
    return (((ca,), (cb,)), ((), ()))


def dot3(ah, al, bh, bl, ca=1, cb=0):
    d = dims(ca, cb)
    out = lax.dot_general(ah, bh, d, preferred_element_type=F32)
    out = out + lax.dot_general(ah, bl, d, preferred_element_type=F32)
    return out + lax.dot_general(al, bh, d, preferred_element_type=F32)


def kernel(
    x, kw, vw, bl, ro, kg, vg,
    go, kvo,
    XP, WH, WL, AH, AL, TT, TS, ST, BS, R, I, T, G, J, GKV, KT, KP, LH, LL, YL, XL, DL, FT, GO, GL, XG, KV,
    bsem, xsem, xbsem, stsem, ktsem, osem,
    ss, rs, kvs, kvr, gs, gr, ps, pr, zs, zr, us, ur,
):
    tok = lax.axis_index("tok")
    feat = lax.axis_index("feat")
    z = lax.rem(tok, 4)
    xlo = lax.div(tok, 4)
    core = lax.rem(feat, 2)
    xhi = lax.rem(lax.div(feat, 2), 2)
    y = lax.div(feat, 4)
    yhi = lax.div(feat, 8)
    yx = lax.rem(feat, 4)
    chip = xhi * 4 + y
    bits = [None, core, xhi, yhi]
    steps = [None, 1, 2, 8]

    def flip(m):
        return (tok, feat + steps[m] - 2 * steps[m] * bits[m])

    core_peer, x_peer = flip(1), flip(2)

    def y_peer(d):
        return (tok, lax.rem(y + d, 4) * 4 + yx)

    def xy_peer(d):
        return (tok, lax.rem(y + d, 4) * 4 + yx + 2 - 4 * xhi)

    def z_peer(d):
        return (xlo * 4 + lax.rem(z + d, 4), feat)

    xlo_peer = (lax.rem(tok + 4, 8), feat)

    def local_copy(src, dst, sem):
        return pltpu.make_async_copy(src, dst, sem)

    def remote(src, dst, s, r, dev):
        return pltpu.make_async_remote_copy(
            src_ref=src, dst_ref=dst, send_sem=s, recv_sem=r, device_id=dev, device_id_type=MESH
        )

    def rows(k, n=CT):
        return pl.ds(pl.multiple_of(k * n, n), n)

    def block_loads(m, slot):
        copies = []
        for i in range(2):
            for j in range(2):
                if m == 0:
                    r0, c0 = i * 128, j * 128
                else:
                    r0 = pl.multiple_of(lax.rem(bits[m] + i, 2) * 128, 128)
                    c0 = pl.multiple_of(lax.rem(bits[m] + j, 2) * 128, 128)
                copies.append(
                    local_copy(
                        bl.at[m, :, pl.ds(r0, 128), pl.ds(c0, 128)],
                        BS.at[pl.ds(4 * slot, 4), 2 * i + j],
                        bsem.at[m],
                    )
                )
        return copies

    def x_loads(k, to, sem_of):
        return [
            local_copy(x.at[pl.ds(k * CT, CT), pl.ds(h * 128, 128)], to(k, h), sem_of(k, h))
            for h in range(8)
        ]

    kt_loads = [
        local_copy(kg, KV.at[pl.ds(0, 64)], ktsem.at[0]),
        local_copy(vg, KV.at[pl.ds(64, 64)], ktsem.at[1]),
    ]
    for cp in kt_loads:
        cp.start()
    first_blocks = block_loads(0, 0)
    for cp in first_blocks:
        cp.start()
    x_copies = [x_loads(k, lambda k, h: XP.at[k // 2, k % 2, h], lambda k, h: xsem.at[k, h]) for k in range(NC)]
    for cp in x_copies[0]:
        cp.start()
    second_blocks = block_loads(1, 1)
    for cp in second_blocks:
        cp.start()
    for k in range(1, NC):
        for cp in x_copies[k]:
            cp.start()

    def w_load(step):
        src = kw if step < 8 else vw
        return local_copy(src.at[pl.ds((step % 8) * 128, 128), :], ST.at[step % 4], stsem.at[step % 4])

    for step in range(4):
        w_load(step).start()

    barrier = pltpu.get_barrier_semaphore()
    peers = [core_peer, x_peer, y_peer(1), y_peer(2), y_peer(3), z_peer(1), z_peer(2), z_peer(3), xlo_peer]
    peers += [xy_peer(1), xy_peer(2), xy_peer(3)]
    for dev in peers:
        pl.semaphore_signal(barrier, inc=1, device_id=dev, device_id_type=MESH)

    for m in range(4):
        order = jnp.broadcast_to(ro[m : m + 1, :], (128, 128))
        hot = (lax.broadcasted_iota(jnp.int32, (128, 128), 0) == order).astype(F32)
        TT[m] = hot.astype(BF16)
        TS[m] = jnp.transpose(hot).astype(BF16)

    corner = pl.ds(0, 128)

    def prepare(m, slot):
        local_copy(bl.at[:, :, corner, corner], BS.at[pl.ds(4 * slot, 4)], bsem.at[m]).wait()
        table = TS[m]

        def one(c, carry):
            for i in range(2):
                for j in range(2):
                    hi, lo = split(BS[4 * slot + c, 2 * i + j])
                    ph = jnp.dot(table, hi, preferred_element_type=F32)
                    p_lo = jnp.dot(table, lo, preferred_element_type=F32)
                    AH[m, c, i * 128 : (i + 1) * 128, j * 128 : (j + 1) * 128] = ph.astype(BF16)
                    AL[m, c, i * 128 : (i + 1) * 128, j * 128 : (j + 1) * 128] = p_lo.astype(BF16)
            return carry

        lax.fori_loop(0, 4, one, 0)

    def fwd_out(m, k):
        return remote(
            R.at[m - 1, 1 - bits[m], :, rows(k)], I.at[m - 1, :, rows(k)],
            ss.at[0, m - 1, 0, k], rs.at[0, m - 1, 0, k], flip(m),
        )

    def fwd_back(m, k):
        return remote(
            T.at[m - 1, :, rows(k)], R.at[m, bits[m], :, rows(k)],
            ss.at[0, m - 1, 1, k], rs.at[0, m - 1, 1, k], flip(m),
        )

    def bwd_out(m, k):
        return remote(
            G.at[m, 1 - bits[m], :, rows(k)], J.at[m - 1, :, rows(k)],
            ss.at[1, m - 1, 0, k], rs.at[1, m - 1, 0, k], flip(m),
        )

    def bwd_back(m, k):
        return remote(
            T.at[3 if m == 2 else m - 1, :, rows(k)], G.at[m - 1, bits[m], :, rows(k)],
            ss.at[1, m - 1, 1, k], rs.at[1, m - 1, 1, k], flip(m),
        )

    def first_factor(k):
        for cp in x_copies[k]:
            cp.wait()
        for u in range(2):
            for c in range(2):
                h = 4 * u + 2 * c
                pair = jnp.concatenate([XP[k // 2, k % 2, h], XP[k // 2, k % 2, h + 1]], axis=1)
                hi, lo = split(pair)
                out = dot3(hi, lo, AH[0, 2 * u + c], AL[0, 2 * u + c])
                R[0, u, 2 * c, k * CT : (k + 1) * CT] = out[:, :128]
                R[0, u, 2 * c + 1, k * CT : (k + 1) * CT] = out[:, 128:]

    def fwd_factor(m, k):
        own = bits[m]

        def one(c, carry):
            pair = jnp.concatenate([R[m - 1, own, c, rows(k)], I[m - 1, c, rows(k)]], axis=1)
            hi, lo = split(pair)
            out = dot3(hi, lo, AH[m, c], AL[m, c])
            R[m, own, c, rows(k)] = out[:, :128]
            T[m - 1, c, rows(k)] = out[:, 128:]
            return carry

        lax.fori_loop(0, 4, one, 0)

    def bwd_factor(m, k):
        own = bits[m]

        def one(c, carry):
            pair = jnp.concatenate([G[m, own, c, rows(k)], J[m - 1, c, rows(k)]], axis=1)
            hi, lo = split(pair)
            out = dot3(hi, lo, AH[m, c], AL[m, c], 1, 1)
            G[m - 1, own, c, rows(k)] = out[:, :128]
            T[3 if m == 2 else m - 1, c, rows(k)] = out[:, 128:]
            return carry

        lax.fori_loop(0, 4, one, 0)

    pair_copy = remote(KT, KP, kvs.at[0], kvr.at[0], core_peer)
    chip_x = (1 - xhi) * 4 + y

    def gx(h):
        return remote(
            GKV.at[core, chip, rows(h, HT)], GKV.at[core, chip, rows(h, HT)],
            kvs.at[1 + h], kvr.at[1 + h], x_peer,
        )

    def gy(d, h, far):
        tile = chip_x if far else chip
        return remote(
            GKV.at[core, tile, rows(h, HT)], GKV.at[core, tile, rows(h, HT)],
            gs.at[far, h], gr.at[far, h], y_peer(d),
        )

    def gy_three(h, far):
        three = GKV.at[core, pl.ds(0, 3), rows(h, HT)]
        return remote(three, three, gs.at[far, h], gr.at[far, h], y_peer(1))

    def gc(h):
        return remote(
            GKV.at[core, :, rows(h, HT)], GKV.at[core, :, rows(h, HT)],
            kvs.at[3 + h], kvr.at[3 + h], core_peer,
        )

    def tiles_send():
        for cp in kt_loads:
            cp.wait()
        KT[...] = jnp.transpose(KV[...])

    def tiles():
        pair_copy.wait_recv()
        lane = lax.broadcasted_iota(jnp.int32, (512, 128), 1)
        mine = (lane < 64) == (core == 0)
        GKV[core, chip] = jnp.where(mine, KT[...], pltpu.roll(KP[...], 64, 1))
        for h in range(2):
            gx(h).start()

    def gather_near(h):
        for d in (1, 3, 2):
            gy(d, h, 0).start()

    def gather_far(h):
        gx(h).wait_recv()
        for d in (1, 3, 2):
            gy(d, h, 1).start()

    def fwd_first(k):
        fwd_out(1, k).wait_recv()
        fwd_factor(1, k)
        fwd_back(1, k).start()

    def weights(part):
        for step in range(2 * part, 2 * part + 2):
            w_load(step).wait()
            s, base = step // 8, (step % 8) * 128

            def strip(i, carry, s=s, base=base, slot=step % 4):
                hi, lo = split(ST[slot, pl.ds(pl.multiple_of(i * 32, 32), 32), :])
                at = pl.ds(pl.multiple_of(base + i * 32, 32), 32)
                for q in range(4):
                    WH[s, q, at, :] = hi[:, q * 256 : (q + 1) * 256]
                    WL[s, q, at, :] = lo[:, q * 256 : (q + 1) * 256]
                return carry

            lax.fori_loop(0, 4, strip, 0)
            if step + 4 < 16:
                w_load(step + 4).start()

    x_again = [x_loads(k, lambda k, h: BS.at[2 * k + h // 4, h % 4], lambda k, h: xbsem.at[k]) for k in range(NC)]

    def gathered(h):
        for far in range(2):
            gy_three(h, far).wait_recv()
        gc(h).start()

    def upstream(h):
        gc(h).wait_recv()
        for s in range(2):
            for t in range(8):
                hi, lo = split(GKV[s, t, h * HT : (h + 1) * HT, :])
                col = (t % 4) * 2 + t // 4
                LH[s, :, col * 128 : (col + 1) * 128] = hi
                LL[s, :, col * 128 : (col + 1) * 128] = lo
        for u in range(2):

            def one(n, carry, u=u):
                at = pl.ds(pl.multiple_of(u * 512 + n * 256, 256), 256)
                acc = None
                for s in range(2):
                    for q in range(4):
                        lh = LH[s, :, q * 256 : (q + 1) * 256]
                        ll = LL[s, :, q * 256 : (q + 1) * 256]
                        part = dot3(lh, ll, WH[s, q, at, :], WL[s, q, at, :], 1, 1)
                        acc = part if acc is None else acc + part
                G[3, u, 2 * n, h * HT : (h + 1) * HT] = acc[:, :128]
                G[3, u, 2 * n + 1, h * HT : (h + 1) * HT] = acc[:, 128:]
                return carry

            lax.fori_loop(0, 2, one, 0)

    def fwd_step(m, k):
        fwd_out(m, k).wait_recv()
        fwd_factor(m, k)
        fwd_back(m, k).start()

    def bwd_step(m, k):
        bwd_out(m, k).wait_recv()
        bwd_factor(m, k)
        bwd_back(m, k).start()

    def fwd_next(m, k):
        fwd_back(m - 1, k).wait_recv()
        fwd_out(m, k).start()

    def bwd_next(m, k):
        bwd_back(m + 1, k).wait_recv()
        bwd_out(m, k).start()

    def gradient(m, t):
        own = 0 if m == 0 else bits[m]

        def one(c, carry):
            if m == 0:
                left = jnp.concatenate(
                    [
                        jnp.concatenate(
                            [BS[2 * k + lax.div(c, 2), 2 * lax.rem(c, 2) + i] for i in range(2)], axis=1
                        )
                        for k in (2 * t, 2 * t + 1)
                    ],
                    axis=0,
                )
                u, base = lax.div(c, 2), 2 * lax.rem(c, 2)
                right = jnp.concatenate([G[0, u, base + i, t * HT : (t + 1) * HT] for i in range(2)], axis=1)
            else:
                at = slice(t * HT, (t + 1) * HT)
                left = jnp.concatenate([R[m - 1, own, c, at], I[m - 1, c, at]], axis=1)
                right = jnp.concatenate([G[m, own, c, at], J[m - 1, c, at]], axis=1)
            lh, ll = split(left)
            rh, rl = split(right)
            total = dot3(lh, ll, rh, rl, 0, 0)
            table = TT[m]
            for i in range(2):
                hi, lo = split(total[i * 128 : (i + 1) * 128])
                back = jnp.dot(table, hi, preferred_element_type=F32) + jnp.dot(
                    table, lo, preferred_element_type=F32
                )
                ii = i if m == 0 else lax.rem(own + i, 2)
                for j in range(2):
                    jj = j if m == 0 else lax.rem(own + j, 2)
                    for zz in range(4):
                        piece = back[zz * 32 : (zz + 1) * 32, j * 128 : (j + 1) * 128]
                        GO[m, zz, ii, c, jj] = piece if t == 0 else GO[m, zz, ii, c, jj] + piece
            return carry

        lax.fori_loop(0, 4, one, 0)
        if t == 1 and m == 0:
            for zz in range(4):
                x_first(zz).start()
        if t == 1 and m > 0:
            for d in (1, 3, 2):
                z_send(m, d).start()

    def x_land(zz):
        return XG.at[0] if zz == 3 else GL.at[0, zz, 1]

    def x_first(zz):
        return remote(
            GO.at[0, zz, 1 - xlo], x_land(zz), zs.at[4], zr.at[4], xlo_peer
        )

    def z_last(d):
        return remote(
            GO.at[0, lax.rem(z + d, 4), xlo], GL.at[0, d - 1, 0], zs.at[0], zr.at[0], z_peer(d)
        )

    def x_sum(m):
        x_four().wait_recv()
        for zz in range(4):
            GO[0, zz, xlo] = GO[0, zz, xlo] + x_land(zz)[...]
        for d in (1, 3, 2):
            z_last(d).start()

    def z_send(m, d):
        return remote(
            GO.at[m, lax.rem(z + d, 4)], GL.at[m, d - 1], zs.at[m], zr.at[m], z_peer(d)
        )

    def z_three(m):
        land = GL.at[m] if m else GL.at[0, :, 0]
        return remote(land, land, zs.at[m], zr.at[m], z_peer(1))

    def x_four():
        land = GO.at[0, :, xlo]
        return remote(land, land, zs.at[4], zr.at[4], xlo_peer)

    def u_send(m):
        return remote(GO.at[m, z, 1 - xlo], XG.at[m], us.at[m], ur.at[m], xlo_peer)

    def z_sum(m):
        z_three(m).wait_recv()
        for side in (1 - xlo, xlo):
            GO[m, z, side] = GO[m, z, side] + GL[m, 0, side] + GL[m, 1, side] + GL[m, 2, side]
        u_send(m).start()

    def share_sum(m):
        if m == 0:
            z_three(0).wait_recv()
            GO[0, z, xlo] = GO[0, z, xlo] + GL[0, 0, 0] + GL[0, 1, 0] + GL[0, 2, 0]
        else:
            u_send(m).wait_recv()
            GO[m, z, xlo] = GO[m, z, xlo] + XG[m]
        result(m).start()

    def result(m):
        return local_copy(GO.at[m, z, xlo], go.at[m], osem.at[m])

    def kv_result(k):
        return local_copy(KV.at[:, rows(k)], kvo.at[:, rows(k)], osem.at[4 + k])

    def p_core(k):
        return remote(
            XP.at[k % 2, 1 - core], GKV.at[0, :, rows(k)], ps.at[k], pr.at[k], core_peer
        )

    def p_x(k):
        return remote(
            XP.at[k % 2, core, pl.ds(4 * (1 - xhi), 4)], XL.at[k], ps.at[8 + k], pr.at[8 + k], x_peer
        )

    def p_y(k, d):
        return remote(
            XP.at[k % 2, core, 4 * xhi + lax.rem(y + d, 4)], YL.at[d - 1, k], ps.at[10 + k], pr.at[10 + k], y_peer(d)
        )

    def p_all(k):
        found = []
        for slot, d, other in ((4, 1, 1), (6, 3, 1), (5, 2, 1), (3, 0, 1), (0, 1, 0), (2, 3, 0), (1, 2, 0)):
            side = 1 - xhi if other else xhi
            dev = (x_peer if d == 0 else xy_peer(d)) if other else y_peer(d)
            found.append(
                remote(
                    XP.at[k % 2, core, 4 * side + lax.rem(y + d, 4)], DL.at[slot, k - 2],
                    ps.at[10 + k], pr.at[10 + k], dev,
                )
            )
        return found

    def p_group(k):
        land = YL.at[:, k] if k < 2 else DL.at[:, k - 2]
        return remote(land, land, ps.at[10 + k], pr.at[10 + k], y_peer(1))

    def p_last(k):
        return remote(FT.at[k], KP.at[rows(k)], ps.at[4 + k], pr.at[4 + k], core_peer)

    def project(k):
        if k >= 2:
            p_core(k - 2).wait_send()
            p_group(k - 2).wait_send()
            p_x(k - 2).wait_send()
        for u in range(2):
            for c in range(4):
                hi, lo = split(R[3, u, c, k * CT : (k + 1) * CT])
                at = slice((u * 4 + c) * 128, (u * 4 + c + 1) * 128)
                LH[0, :CT, at] = hi
                LL[0, :CT, at] = lo
        for s in range(2):

            def one(n, carry, s=s):
                out = dot3(LH[0, :CT, :], LL[0, :CT, :], WH[s, n], WL[s, n])
                XP[k % 2, s, n] = out[:, :128]
                XP[k % 2, s, 4 + n] = out[:, 128:]
                return carry

            lax.fori_loop(0, 4, one, 0)
        p_core(k).start()

    def project_y(k):
        p_core(k).wait_recv()

        def one(t, carry):
            XP[k % 2, core, t] = XP[k % 2, core, t] + GKV[0, t, k * CT : (k + 1) * CT]
            return carry

        lax.fori_loop(0, 8, one, 0)
        if k < 2:
            p_x(k).start()
        else:
            for cp in p_all(k):
                cp.start()

    def project_x(k):
        p_x(k).wait_recv()
        for t in range(4):
            XP[k % 2, core, 4 * xhi + t] = XP[k % 2, core, 4 * xhi + t] + XL[k, t]
        for d in (1, 3, 2):
            p_y(k, d).start()

    def project_last(k):
        total = None
        if k < 2:
            p_group(k).wait_recv()
            total = XP[k % 2, core, chip] + YL[0, k] + YL[1, k] + YL[2, k]
        else:
            p_group(k).wait_recv()
            total = XP[k % 2, core, chip]
            for slot in range(7):
                total = total + DL[slot, k - 2]
        FT[k] = total
        p_last(k).start()

    def project_out(k):
        p_last(k).wait_recv()
        at = slice(k * CT, (k + 1) * CT)
        key_tile = jnp.where(core == 0, FT[k], KP[at])
        value_tile = jnp.where(core == 0, KP[at], FT[k])
        key_tile = jnp.transpose(key_tile)
        value_tile = jnp.transpose(value_tile)
        KV[:64, at] = jnp.where(core == 0, key_tile[:64], key_tile[64:])
        KV[64:, at] = jnp.where(core == 0, value_tile[:64], value_tile[64:])
        kv_result(k).start()

    def fwd_last(k):
        bwd_back(3, k).wait_send()
        fwd_step(3, k)

    def bwd_mid(k):
        bwd_step(2, k)

    def bwd_low(k):
        fwd_back(1, k).wait_send()
        bwd_step(1, k)

    def gather_done():
        for h in range(2):
            gx(h).wait_send()
            gc(h).wait_send()
            for far in range(2):
                gy_three(h, far).wait_send()

    def bwd_low_out(k):
        if k == 0:
            gather_done()
        bwd_next(1, k)

    def bwd_grad0(t):
        for k in (2 * t, 2 * t + 1):
            bwd_back(1, k).wait_recv()
            local_copy(
                bl.at[pl.ds(0, 2), :, corner, corner], BS.at[pl.ds(2 * k, 2)], xbsem.at[k]
            ).wait()
        gradient(0, t)

    def project_in(k):
        fwd_back(3, k).wait_recv()
        project(k)

    def late_prepare(m):
        prepare(m, m % 2)
        if m == 3:
            for group in x_again:
                for cp in group:
                    cp.start()

    steps_of = {
        "Q": late_prepare,
        "T": tiles,
        "X": gather_far,
        "TY": gather_near,
        "Z": gathered,
        "W": weights,
        "H": upstream,
        "HS": lambda k: bwd_out(3, k).start(),
        "B": fwd_first,
        "C": lambda k: fwd_next(2, k),
        "D": lambda k: fwd_step(2, k),
        "E": lambda k: fwd_next(3, k),
        "F": fwd_last,
        "I": lambda k: bwd_step(3, k),
        "J": lambda k: bwd_next(2, k),
        "K": bwd_mid,
        "L": bwd_low_out,
        "M": bwd_low,
        "G": gradient,
        "N": bwd_grad0,
        "P": project_in,
        "PY": project_y,
        "PX": project_x,
        "PL": project_last,
        "PO": project_out,
        "S": z_sum,
        "SX": x_sum,
        "U": share_sum,
    }

    tiles_send()
    prepare(0, 0)
    third_blocks = block_loads(2, 0)
    for cp in third_blocks:
        cp.start()
    for k in range(NC):
        first_factor(k)
    prepare(1, 1)
    fourth_blocks = block_loads(3, 1)
    for cp in fourth_blocks:
        cp.start()
    pl.semaphore_wait(barrier, len(peers))
    pair_copy.start()
    for k in range(NC):
        fwd_out(1, k).start()

    for name, *args in ORDER:
        steps_of[name](*args)

    def sends_end():
        for m in (1, 2, 3):
            for k in range(NC):
                fwd_out(m, k).wait_send()
                bwd_out(m, k).wait_send()
        for k in range(NC):
            fwd_back(3, k).wait_send()
            fwd_back(2, k).wait_send()
            bwd_back(2, k).wait_send()
            bwd_back(1, k).wait_send()
            p_last(k).wait_send()
        for k in (2, 3):
            p_core(k).wait_send()
            p_group(k).wait_send()
        pair_copy.wait_send()
        for m in range(4):
            z_three(m).wait_send()
            if m:
                u_send(m).wait_send()
            result(m).wait()
        x_four().wait_send()
        for k in range(NC):
            kv_result(k).wait()

    sends_end()


def finish(g, kv, mo, se, bl, ko, vo, nb, nm, ns, GV, KB, A, isem, jsem, osem):
    tok = lax.axis_index("tok")
    share = pl.ds(pl.multiple_of(tok * 32, 32), 32)
    copy = pltpu.make_async_copy

    def loads(m):
        return [
            copy(g.at[m], GV.at[m], isem.at[0, m]),
            copy(mo.at[m], A.at[0, m], isem.at[1, m]),
            copy(se.at[m], A.at[1, m], isem.at[2, m]),
            copy(bl.at[m, :, share, :], A.at[2, m], isem.at[3, m]),
        ]

    def stores(m):
        return [copy(A.at[i, m], out.at[m], osem.at[i, m]) for i, out in enumerate((nm, ns, nb))]

    kv_load = copy(kv, KB, jsem.at[0])
    kv_load.start()
    every = [loads(m) for m in range(4)]
    for group in every:
        for cp in group:
            cp.start()
    kv_load.wait()
    kv_stores = [
        copy(KB.at[pl.ds(0, 64)], ko, jsem.at[1]),
        copy(KB.at[pl.ds(64, 64)], vo, jsem.at[2]),
    ]
    for cp in kv_stores:
        cp.start()
    for m in range(4):
        for cp in every[m]:
            cp.wait()
        for c in range(4):
            for j in range(2):
                at = slice(j * 128, (j + 1) * 128)
                grad = GV[m, c, j]
                moment = beta_one * A[0, m, c, :, at] + (1.0 - beta_one) * grad
                second = beta_two * A[1, m, c, :, at] + (1.0 - beta_two) * grad * grad
                step = learn_rate * (moment / bias_one) / (jnp.sqrt(second / bias_two) + epsilon)
                A[0, m, c, :, at] = moment
                A[1, m, c, :, at] = second
                A[2, m, c, :, at] = A[2, m, c, :, at] - step
        for cp in stores(m):
            cp.start()
    for m in range(4):
        for cp in stores(m):
            cp.wait()
    for cp in kv_stores:
        cp.wait()


def local(x, kw, vw, bl, ro, kg, vg, mo, se):
    hbm = pl.BlockSpec(memory_space=pl.ANY)
    vmem = pl.BlockSpec(memory_space=pltpu.VMEM)
    dma = pltpu.SemaphoreType.DMA
    tile = (128, 128)
    scratch = [
        pltpu.VMEM((2, 2, 8) + tile, F32),
        pltpu.VMEM((2, 4, 1024, 256), BF16),
        pltpu.VMEM((2, 4, 1024, 256), BF16),
        pltpu.VMEM((4, 4, 256, 256), BF16),
        pltpu.VMEM((4, 4, 256, 256), BF16),
        pltpu.VMEM((4,) + tile, BF16),
        pltpu.VMEM((4,) + tile, BF16),
        pltpu.VMEM((4, 128, 1024), F32),
        pltpu.VMEM((8, 4) + tile, F32),
        pltpu.VMEM((4, 2, 4, 512, 128), F32),
        pltpu.VMEM((3, 4, 512, 128), F32),
        pltpu.VMEM((4, 4, 512, 128), F32),
        pltpu.VMEM((4, 2, 4, 512, 128), F32),
        pltpu.VMEM((3, 4, 512, 128), F32),
        pltpu.VMEM((2, 8, 512, 128), F32),
        pltpu.VMEM((512, 128), F32),
        pltpu.VMEM((512, 128), F32),
        pltpu.VMEM((2, 256, 1024), BF16),
        pltpu.VMEM((2, 256, 1024), BF16),
        pltpu.VMEM((3, 2) + tile, F32),
        pltpu.VMEM((2, 4) + tile, F32),
        pltpu.VMEM((7, 2) + tile, F32),
        pltpu.VMEM((4,) + tile, F32),
        pltpu.VMEM((4, 4, 2, 4, 2, 32, 128), F32),
        pltpu.VMEM((4, 3, 2, 4, 2, 32, 128), F32),
        pltpu.VMEM((4, 4, 2, 32, 128), F32),
        pltpu.VMEM((128, 512), F32),
        dma((4,)),
        dma((4, 8)),
        dma((4,)),
        dma((4,)),
        dma((2,)),
        dma((8,)),
        dma((2, 3, 2, 4)),
        dma((2, 3, 2, 4)),
        dma((5,)),
        dma((5,)),
        dma((2, 2)),
        dma((2, 2)),
        dma((14,)),
        dma((14,)),
        dma((5,)),
        dma((5,)),
        dma((4,)),
        dma((4,)),
    ]
    share = jax.ShapeDtypeStruct((4, 4, 32, 256), F32)
    narrow = jax.ShapeDtypeStruct((64, 512), F32)
    grads, kv = pl.pallas_call(
        kernel,
        out_shape=(
            jax.ShapeDtypeStruct((4, 4, 2, 32, 128), F32),
            jax.ShapeDtypeStruct((128, 512), F32),
        ),
        in_specs=[hbm, hbm, hbm, hbm, vmem, hbm, hbm],
        out_specs=(hbm, hbm),
        scratch_shapes=scratch,
        compiler_params=pltpu.CompilerParams(
            collective_id=0, has_side_effects=True, vmem_limit_bytes=67043328
        ),
    )(x, kw, vw, bl, ro, kg.T, vg.T)
    ko, vo, nb, nm, ns = pl.pallas_call(
        finish,
        out_shape=(narrow, narrow, share, share, share),
        in_specs=[hbm] * 5,
        out_specs=(hbm,) * 5,
        scratch_shapes=[
            pltpu.VMEM((4, 4, 2, 32, 128), F32),
            pltpu.VMEM((128, 512), F32),
            pltpu.VMEM((3, 4, 4, 32, 256), F32),
            dma((4, 4)),
            dma((3,)),
            dma((3, 4)),
        ],
    )(grads, kv, mo, se, bl)
    return ko.T, vo.T, nb, nm, ns


def solution(mesh):
    placed = (
        P("tok", "feat"),
        P("feat", None),
        P("feat", None),
        P(None, "feat", None, None),
        P(),
        P("tok", "feat"),
        P("tok", "feat"),
        P(None, "feat", "tok", None),
        P(None, "feat", "tok", None),
    )
    return jax.shard_map(
        local,
        mesh=mesh,
        in_specs=placed,
        out_specs=(
            P("tok", "feat"),
            P("tok", "feat"),
            P(None, "feat", "tok", None),
            P(None, "feat", "tok", None),
            P(None, "feat", "tok", None),
        ),
        check_vma=False,
    )
```

```python
import jax
import jax.numpy as jnp
from jax import lax
from jax.experimental import pallas as pl
from jax.experimental.pallas import tpu as pltpu
from jax.sharding import PartitionSpec as P

MESH = pl.DeviceIdType.MESH
F32 = jnp.float32
BF16 = jnp.bfloat16
beta_one = 0.9
beta_two = 0.95
learn_rate = 0.01
epsilon = 1e-08
bias_one = 1.0 - 0.9**10
bias_two = 1.0 - 0.95**10

ORDER = (
    ("W", 0), ("T",), ("TY", 0), ("B", 2), ("B", 0), ("Q", 2), ("C", 0), ("X", 0), ("Q", 3),
    ("B", 1), ("W", 1), ("B", 3), ("W", 2), ("W", 3), ("C", 2), ("C", 1), ("X", 1), ("W", 4),
    ("W", 5), ("Z", 0), ("D", 0), ("W", 6), ("W", 7), ("TY", 1), ("H", 0), ("HS", 0), ("D", 2),
    ("Z", 1), ("HS", 1), ("D", 1), ("C", 3), ("I", 0), ("I", 1), ("H", 1), ("J", 0), ("HS", 2),
    ("HS", 3), ("J", 1), ("K", 0), ("I", 2), ("K", 1), ("I", 3), ("L", 0), ("J", 2), ("E", 0),
    ("M", 0), ("E", 1), ("G", 2, 0), ("L", 1), ("J", 3), ("M", 1), ("G", 1, 0), ("K", 2), ("F", 0),
    ("D", 3), ("N", 0), ("K", 3), ("F", 1), ("E", 2), ("G", 2, 1), ("L", 2), ("P", 0), ("M", 2),
    ("PY", 0), ("E", 3), ("P", 1), ("L", 3), ("PY", 1), ("F", 2), ("M", 3), ("S", 2), ("G", 1, 1),
    ("PX", 0), ("F", 3), ("N", 1), ("PX", 1), ("G", 3, 0), ("U", 2), ("G", 3, 1), ("PL", 0),
    ("P", 2), ("PO", 0), ("S", 1), ("PY", 2), ("PL", 1), ("P", 3), ("SX", 0), ("U", 1), ("PY", 3),
    ("S", 3), ("PL", 2), ("U", 0), ("PO", 1), ("PL", 3), ("U", 3), ("PO", 2), ("PO", 3),
)

CT = 128
NC = 4
HT = 256


def split(v):
    hi = v.astype(BF16)
    lo = (v - hi.astype(F32)).astype(BF16)
    return hi, lo


def dims(ca, cb):
    return (((ca,), (cb,)), ((), ()))


def dot3(ah, al, bh, bl, ca=1, cb=0):
    d = dims(ca, cb)
    out = lax.dot_general(ah, bh, d, preferred_element_type=F32)
    out = out + lax.dot_general(ah, bl, d, preferred_element_type=F32)
    return out + lax.dot_general(al, bh, d, preferred_element_type=F32)


def kernel(
    x, kw, vw, bl, ro, kg, vg,
    go, kvo,
    XP, WH, WL, AH, AL, TT, TS, ST, BS, R, I, T, G, J, GKV, KT, KP, LH, LL, YL, XL, DL, FT, GO, GL, XG, KV,
    bsem, xsem, xbsem, stsem, ktsem, osem,
    ss, rs, kvs, kvr, gs, gr, ps, pr, zs, zr, us, ur,
):
    tok = lax.axis_index("tok")
    feat = lax.axis_index("feat")
    z = lax.rem(tok, 4)
    xlo = lax.div(tok, 4)
    core = lax.rem(feat, 2)
    xhi = lax.rem(lax.div(feat, 2), 2)
    y = lax.div(feat, 4)
    yhi = lax.div(feat, 8)
    yx = lax.rem(feat, 4)
    chip = xhi * 4 + y
    bits = [None, core, xhi, yhi]
    steps = [None, 1, 2, 8]

    def flip(m):
        return (tok, feat + steps[m] - 2 * steps[m] * bits[m])

    core_peer, x_peer = flip(1), flip(2)

    def y_peer(d):
        return (tok, lax.rem(y + d, 4) * 4 + yx)

    def xy_peer(d):
        return (tok, lax.rem(y + d, 4) * 4 + yx + 2 - 4 * xhi)

    def z_peer(d):
        return (xlo * 4 + lax.rem(z + d, 4), feat)

    xlo_peer = (lax.rem(tok + 4, 8), feat)

    def local_copy(src, dst, sem):
        return pltpu.make_async_copy(src, dst, sem)

    def remote(src, dst, s, r, dev):
        return pltpu.make_async_remote_copy(
            src_ref=src, dst_ref=dst, send_sem=s, recv_sem=r, device_id=dev, device_id_type=MESH
        )

    def rows(k, n=CT):
        return pl.ds(pl.multiple_of(k * n, n), n)

    def block_loads(m, slot):
        copies = []
        for i in range(2):
            for j in range(2):
                if m == 0:
                    r0, c0 = i * 128, j * 128
                else:
                    r0 = pl.multiple_of(lax.rem(bits[m] + i, 2) * 128, 128)
                    c0 = pl.multiple_of(lax.rem(bits[m] + j, 2) * 128, 128)
                copies.append(
                    local_copy(
                        bl.at[m, :, pl.ds(r0, 128), pl.ds(c0, 128)],
                        BS.at[pl.ds(4 * slot, 4), 2 * i + j],
                        bsem.at[m],
                    )
                )
        return copies

    def x_loads(k, to, sem_of):
        return [
            local_copy(x.at[pl.ds(k * CT, CT), pl.ds(h * 128, 128)], to(k, h), sem_of(k, h))
            for h in range(8)
        ]

    kt_loads = [
        local_copy(kg, KV.at[pl.ds(0, 64)], ktsem.at[0]),
        local_copy(vg, KV.at[pl.ds(64, 64)], ktsem.at[1]),
    ]
    for cp in kt_loads:
        cp.start()
    first_blocks = block_loads(0, 0)
    for cp in first_blocks:
        cp.start()
    x_copies = [x_loads(k, lambda k, h: XP.at[k // 2, k % 2, h], lambda k, h: xsem.at[k, h]) for k in range(NC)]
    for cp in x_copies[0]:
        cp.start()
    second_blocks = block_loads(1, 1)
    for cp in second_blocks:
        cp.start()
    for k in range(1, NC):
        for cp in x_copies[k]:
            cp.start()

    def w_load(step):
        src = kw if step < 8 else vw
        return local_copy(src.at[pl.ds((step % 8) * 128, 128), :], ST.at[step % 4], stsem.at[step % 4])

    for step in range(4):
        w_load(step).start()

    barrier = pltpu.get_barrier_semaphore()
    peers = [core_peer, x_peer, y_peer(1), y_peer(2), y_peer(3), z_peer(1), z_peer(2), z_peer(3), xlo_peer]
    peers += [xy_peer(1), xy_peer(2), xy_peer(3)]
    for dev in peers:
        pl.semaphore_signal(barrier, inc=1, device_id=dev, device_id_type=MESH)

    for m in range(4):
        order = jnp.broadcast_to(ro[m : m + 1, :], (128, 128))
        hot = (lax.broadcasted_iota(jnp.int32, (128, 128), 0) == order).astype(F32)
        TT[m] = hot.astype(BF16)
        TS[m] = jnp.transpose(hot).astype(BF16)

    corner = pl.ds(0, 128)

    def prepare(m, slot):
        local_copy(bl.at[:, :, corner, corner], BS.at[pl.ds(4 * slot, 4)], bsem.at[m]).wait()
        table = TS[m]

        def one(c, carry):
            for i in range(2):
                for j in range(2):
                    hi, lo = split(BS[4 * slot + c, 2 * i + j])
                    ph = jnp.dot(table, hi, preferred_element_type=F32)
                    p_lo = jnp.dot(table, lo, preferred_element_type=F32)
                    AH[m, c, i * 128 : (i + 1) * 128, j * 128 : (j + 1) * 128] = ph.astype(BF16)
                    AL[m, c, i * 128 : (i + 1) * 128, j * 128 : (j + 1) * 128] = p_lo.astype(BF16)
            return carry

        lax.fori_loop(0, 4, one, 0)

    def fwd_out(m, k):
        return remote(
            R.at[m - 1, 1 - bits[m], :, rows(k)], I.at[m - 1, :, rows(k)],
            ss.at[0, m - 1, 0], rs.at[0, m - 1, 0, k], flip(m),
        )

    def fwd_back(m, k):
        return remote(
            T.at[m - 1, :, rows(k)], R.at[m, bits[m], :, rows(k)],
            ss.at[0, m - 1, 1], rs.at[0, m - 1, 1, k], flip(m),
        )

    def bwd_out(m, k):
        return remote(
            G.at[m, 1 - bits[m], :, rows(k)], J.at[m - 1, :, rows(k)],
            ss.at[1, m - 1, 0], rs.at[1, m - 1, 0, k], flip(m),
        )

    def bwd_back(m, k):
        return remote(
            T.at[3 if m == 2 else m - 1, :, rows(k)], G.at[m - 1, bits[m], :, rows(k)],
            ss.at[1, m - 1, 1], rs.at[1, m - 1, 1, k], flip(m),
        )

    def all_sent(way, m, back):
        return remote(I.at[m - 1], I.at[m - 1], ss.at[way, m - 1, back], rs.at[way, m - 1, back, 0], flip(m))

    sent = []

    def wait_all_sent(way, m, back):
        if (way, m, back) not in sent:
            sent.append((way, m, back))
            all_sent(way, m, back).wait_send()

    def first_factor(k):
        for cp in x_copies[k]:
            cp.wait()
        for u in range(2):
            for c in range(2):
                h = 4 * u + 2 * c
                pair = jnp.concatenate([XP[k // 2, k % 2, h], XP[k // 2, k % 2, h + 1]], axis=1)
                hi, lo = split(pair)
                out = dot3(hi, lo, AH[0, 2 * u + c], AL[0, 2 * u + c])
                R[0, u, 2 * c, k * CT : (k + 1) * CT] = out[:, :128]
                R[0, u, 2 * c + 1, k * CT : (k + 1) * CT] = out[:, 128:]

    def fwd_factor(m, k):
        own = bits[m]

        def one(c, carry):
            pair = jnp.concatenate([R[m - 1, own, c, rows(k)], I[m - 1, c, rows(k)]], axis=1)
            hi, lo = split(pair)
            out = dot3(hi, lo, AH[m, c], AL[m, c])
            R[m, own, c, rows(k)] = out[:, :128]
            T[m - 1, c, rows(k)] = out[:, 128:]
            return carry

        lax.fori_loop(0, 4, one, 0)

    def bwd_factor(m, k):
        own = bits[m]

        def one(c, carry):
            pair = jnp.concatenate([G[m, own, c, rows(k)], J[m - 1, c, rows(k)]], axis=1)
            hi, lo = split(pair)
            out = dot3(hi, lo, AH[m, c], AL[m, c], 1, 1)
            G[m - 1, own, c, rows(k)] = out[:, :128]
            T[3 if m == 2 else m - 1, c, rows(k)] = out[:, 128:]
            return carry

        lax.fori_loop(0, 4, one, 0)

    pair_copy = remote(KT, KP, kvs.at[0], kvr.at[0], core_peer)
    chip_x = (1 - xhi) * 4 + y

    def gx(h):
        return remote(
            GKV.at[core, chip, rows(h, HT)], GKV.at[core, chip, rows(h, HT)],
            kvs.at[1 + h], kvr.at[1 + h], x_peer,
        )

    def gy(d, h, far):
        tile = chip_x if far else chip
        return remote(
            GKV.at[core, tile, rows(h, HT)], GKV.at[core, tile, rows(h, HT)],
            gs.at[far, h], gr.at[far, h], y_peer(d),
        )

    def gy_three(h, far):
        three = GKV.at[core, pl.ds(0, 3), rows(h, HT)]
        return remote(three, three, gs.at[far, h], gr.at[far, h], y_peer(1))

    def gc(h):
        return remote(
            GKV.at[core, :, rows(h, HT)], GKV.at[core, :, rows(h, HT)],
            kvs.at[3 + h], kvr.at[3 + h], core_peer,
        )

    def tiles_send():
        for cp in kt_loads:
            cp.wait()
        KT[...] = jnp.transpose(KV[...])

    def tiles():
        pair_copy.wait_recv()
        lane = lax.broadcasted_iota(jnp.int32, (512, 128), 1)
        mine = (lane < 64) == (core == 0)
        GKV[core, chip] = jnp.where(mine, KT[...], pltpu.roll(KP[...], 64, 1))
        for h in range(2):
            gx(h).start()

    def gather_near(h):
        for d in (1, 3, 2):
            gy(d, h, 0).start()

    def gather_far(h):
        gx(h).wait_recv()
        for d in (1, 3, 2):
            gy(d, h, 1).start()

    def fwd_first(k):
        fwd_out(1, k).wait_recv()
        fwd_factor(1, k)
        fwd_back(1, k).start()

    def weights(part):
        for step in range(2 * part, 2 * part + 2):
            w_load(step).wait()
            s, base = step // 8, (step % 8) * 128

            def strip(i, carry, s=s, base=base, slot=step % 4):
                hi, lo = split(ST[slot, pl.ds(pl.multiple_of(i * 32, 32), 32), :])
                at = pl.ds(pl.multiple_of(base + i * 32, 32), 32)
                for q in range(4):
                    WH[s, q, at, :] = hi[:, q * 256 : (q + 1) * 256]
                    WL[s, q, at, :] = lo[:, q * 256 : (q + 1) * 256]
                return carry

            lax.fori_loop(0, 4, strip, 0)
            if step + 4 < 16:
                w_load(step + 4).start()

    x_again = [x_loads(k, lambda k, h: BS.at[2 * k + h // 4, h % 4], lambda k, h: xbsem.at[k]) for k in range(NC)]

    def gathered(h):
        for far in range(2):
            gy_three(h, far).wait_recv()
        gc(h).start()

    def upstream(h):
        gc(h).wait_recv()
        for s in range(2):
            for t in range(8):
                hi, lo = split(GKV[s, t, h * HT : (h + 1) * HT, :])
                col = (t % 4) * 2 + t // 4
                LH[s, :, col * 128 : (col + 1) * 128] = hi
                LL[s, :, col * 128 : (col + 1) * 128] = lo
        for u in range(2):

            def one(n, carry, u=u):
                at = pl.ds(pl.multiple_of(u * 512 + n * 256, 256), 256)
                acc = None
                for s in range(2):
                    for q in range(4):
                        lh = LH[s, :, q * 256 : (q + 1) * 256]
                        ll = LL[s, :, q * 256 : (q + 1) * 256]
                        part = dot3(lh, ll, WH[s, q, at, :], WL[s, q, at, :], 1, 1)
                        acc = part if acc is None else acc + part
                G[3, u, 2 * n, h * HT : (h + 1) * HT] = acc[:, :128]
                G[3, u, 2 * n + 1, h * HT : (h + 1) * HT] = acc[:, 128:]
                return carry

            lax.fori_loop(0, 2, one, 0)

    def fwd_step(m, k):
        fwd_out(m, k).wait_recv()
        fwd_factor(m, k)
        fwd_back(m, k).start()

    def bwd_step(m, k):
        bwd_out(m, k).wait_recv()
        bwd_factor(m, k)
        bwd_back(m, k).start()

    def fwd_next(m, k):
        fwd_back(m - 1, k).wait_recv()
        fwd_out(m, k).start()

    def bwd_next(m, k):
        bwd_back(m + 1, k).wait_recv()
        bwd_out(m, k).start()

    def gradient(m, t):
        own = 0 if m == 0 else bits[m]

        def one(c, carry):
            if m == 0:
                left = jnp.concatenate(
                    [
                        jnp.concatenate(
                            [BS[2 * k + lax.div(c, 2), 2 * lax.rem(c, 2) + i] for i in range(2)], axis=1
                        )
                        for k in (2 * t, 2 * t + 1)
                    ],
                    axis=0,
                )
                u, base = lax.div(c, 2), 2 * lax.rem(c, 2)
                right = jnp.concatenate([G[0, u, base + i, t * HT : (t + 1) * HT] for i in range(2)], axis=1)
            else:
                at = slice(t * HT, (t + 1) * HT)
                left = jnp.concatenate([R[m - 1, own, c, at], I[m - 1, c, at]], axis=1)
                right = jnp.concatenate([G[m, own, c, at], J[m - 1, c, at]], axis=1)
            lh, ll = split(left)
            rh, rl = split(right)
            total = dot3(lh, ll, rh, rl, 0, 0)
            table = TT[m]
            for i in range(2):
                hi, lo = split(total[i * 128 : (i + 1) * 128])
                back = jnp.dot(table, hi, preferred_element_type=F32) + jnp.dot(
                    table, lo, preferred_element_type=F32
                )
                ii = i if m == 0 else lax.rem(own + i, 2)
                for j in range(2):
                    jj = j if m == 0 else lax.rem(own + j, 2)
                    for zz in range(4):
                        piece = back[zz * 32 : (zz + 1) * 32, j * 128 : (j + 1) * 128]
                        GO[m, zz, ii, c, jj] = piece if t == 0 else GO[m, zz, ii, c, jj] + piece
            return carry

        lax.fori_loop(0, 4, one, 0)
        if t == 1 and m == 0:
            for zz in range(4):
                x_first(zz).start()
        if t == 1 and m > 0:
            for d in (1, 3, 2):
                z_send(m, d).start()

    def x_land(zz):
        return XG.at[0] if zz == 3 else GL.at[0, zz, 1]

    def x_first(zz):
        return remote(
            GO.at[0, zz, 1 - xlo], x_land(zz), zs.at[4], zr.at[4], xlo_peer
        )

    def z_last(d):
        return remote(
            GO.at[0, lax.rem(z + d, 4), xlo], GL.at[0, d - 1, 0], zs.at[0], zr.at[0], z_peer(d)
        )

    def x_sum(m):
        x_four().wait_recv()
        for zz in range(4):
            GO[0, zz, xlo] = GO[0, zz, xlo] + x_land(zz)[...]
        for d in (1, 3, 2):
            z_last(d).start()

    def z_send(m, d):
        return remote(
            GO.at[m, lax.rem(z + d, 4)], GL.at[m, d - 1], zs.at[m], zr.at[m], z_peer(d)
        )

    def z_three(m):
        land = GL.at[m] if m else GL.at[0, :, 0]
        return remote(land, land, zs.at[m], zr.at[m], z_peer(1))

    def x_four():
        land = GO.at[0, :, xlo]
        return remote(land, land, zs.at[4], zr.at[4], xlo_peer)

    def u_send(m):
        return remote(GO.at[m, z, 1 - xlo], XG.at[m], us.at[m], ur.at[m], xlo_peer)

    def z_sum(m):
        z_three(m).wait_recv()
        for side in (1 - xlo, xlo):
            GO[m, z, side] = GO[m, z, side] + GL[m, 0, side] + GL[m, 1, side] + GL[m, 2, side]
        u_send(m).start()

    def share_sum(m):
        if m == 0:
            z_three(0).wait_recv()
            GO[0, z, xlo] = GO[0, z, xlo] + GL[0, 0, 0] + GL[0, 1, 0] + GL[0, 2, 0]
        else:
            u_send(m).wait_recv()
            GO[m, z, xlo] = GO[m, z, xlo] + XG[m]
        result(m).start()

    def result(m):
        return local_copy(GO.at[m, z, xlo], go.at[m], osem.at[m])

    def kv_result(k):
        return local_copy(KV.at[:, rows(k)], kvo.at[:, rows(k)], osem.at[4 + k])

    def p_core(k):
        return remote(
            XP.at[k % 2, 1 - core], GKV.at[0, :, rows(k)], ps.at[k], pr.at[k], core_peer
        )

    def p_x(k):
        return remote(
            XP.at[k % 2, core, pl.ds(4 * (1 - xhi), 4)], XL.at[k], ps.at[8 + k], pr.at[8 + k], x_peer
        )

    def p_y(k, d):
        return remote(
            XP.at[k % 2, core, 4 * xhi + lax.rem(y + d, 4)], YL.at[d - 1, k], ps.at[10 + k], pr.at[10 + k], y_peer(d)
        )

    def p_all(k):
        found = []
        for slot, d, other in ((4, 1, 1), (6, 3, 1), (5, 2, 1), (3, 0, 1), (0, 1, 0), (2, 3, 0), (1, 2, 0)):
            side = 1 - xhi if other else xhi
            dev = (x_peer if d == 0 else xy_peer(d)) if other else y_peer(d)
            found.append(
                remote(
                    XP.at[k % 2, core, 4 * side + lax.rem(y + d, 4)], DL.at[slot, k - 2],
                    ps.at[10 + k], pr.at[10 + k], dev,
                )
            )
        return found

    def p_group(k):
        land = YL.at[:, k] if k < 2 else DL.at[:, k - 2]
        return remote(land, land, ps.at[10 + k], pr.at[10 + k], y_peer(1))

    def p_last(k):
        return remote(FT.at[k], KP.at[rows(k)], ps.at[4 + k], pr.at[4 + k], core_peer)

    def project(k):
        if k >= 2:
            p_core(k - 2).wait_send()
            p_group(k - 2).wait_send()
            p_x(k - 2).wait_send()
        for u in range(2):
            for c in range(4):
                hi, lo = split(R[3, u, c, k * CT : (k + 1) * CT])
                at = slice((u * 4 + c) * 128, (u * 4 + c + 1) * 128)
                LH[0, :CT, at] = hi
                LL[0, :CT, at] = lo
        for s in range(2):

            def one(n, carry, s=s):
                out = dot3(LH[0, :CT, :], LL[0, :CT, :], WH[s, n], WL[s, n])
                XP[k % 2, s, n] = out[:, :128]
                XP[k % 2, s, 4 + n] = out[:, 128:]
                return carry

            lax.fori_loop(0, 4, one, 0)
        p_core(k).start()

    def project_y(k):
        p_core(k).wait_recv()

        def one(t, carry):
            XP[k % 2, core, t] = XP[k % 2, core, t] + GKV[0, t, k * CT : (k + 1) * CT]
            return carry

        lax.fori_loop(0, 8, one, 0)
        if k < 2:
            p_x(k).start()
        else:
            for cp in p_all(k):
                cp.start()

    def project_x(k):
        p_x(k).wait_recv()
        for t in range(4):
            XP[k % 2, core, 4 * xhi + t] = XP[k % 2, core, 4 * xhi + t] + XL[k, t]
        for d in (1, 3, 2):
            p_y(k, d).start()

    def project_last(k):
        total = None
        if k < 2:
            p_group(k).wait_recv()
            total = XP[k % 2, core, chip] + YL[0, k] + YL[1, k] + YL[2, k]
        else:
            p_group(k).wait_recv()
            total = XP[k % 2, core, chip]
            for slot in range(7):
                total = total + DL[slot, k - 2]
        FT[k] = total
        p_last(k).start()

    def project_out(k):
        p_last(k).wait_recv()
        at = slice(k * CT, (k + 1) * CT)
        key_tile = jnp.where(core == 0, FT[k], KP[at])
        value_tile = jnp.where(core == 0, KP[at], FT[k])
        key_tile = jnp.transpose(key_tile)
        value_tile = jnp.transpose(value_tile)
        KV[:64, at] = jnp.where(core == 0, key_tile[:64], key_tile[64:])
        KV[64:, at] = jnp.where(core == 0, value_tile[:64], value_tile[64:])
        kv_result(k).start()

    def fwd_last(k):
        wait_all_sent(1, 3, 1)
        fwd_step(3, k)

    def bwd_mid(k):
        bwd_step(2, k)

    def bwd_low(k):
        wait_all_sent(0, 1, 1)
        bwd_step(1, k)

    def gather_done():
        for h in range(2):
            gx(h).wait_send()
            gc(h).wait_send()
            for far in range(2):
                gy_three(h, far).wait_send()

    def bwd_low_out(k):
        if k == 0:
            gather_done()
        bwd_next(1, k)

    def bwd_grad0(t):
        for k in (2 * t, 2 * t + 1):
            bwd_back(1, k).wait_recv()
            local_copy(
                bl.at[pl.ds(0, 2), :, corner, corner], BS.at[pl.ds(2 * k, 2)], xbsem.at[k]
            ).wait()
        gradient(0, t)

    def project_in(k):
        fwd_back(3, k).wait_recv()
        project(k)

    def late_prepare(m):
        prepare(m, m % 2)
        if m == 3:
            for group in x_again:
                for cp in group:
                    cp.start()

    steps_of = {
        "Q": late_prepare,
        "T": tiles,
        "X": gather_far,
        "TY": gather_near,
        "Z": gathered,
        "W": weights,
        "H": upstream,
        "HS": lambda k: bwd_out(3, k).start(),
        "B": fwd_first,
        "C": lambda k: fwd_next(2, k),
        "D": lambda k: fwd_step(2, k),
        "E": lambda k: fwd_next(3, k),
        "F": fwd_last,
        "I": lambda k: bwd_step(3, k),
        "J": lambda k: bwd_next(2, k),
        "K": bwd_mid,
        "L": bwd_low_out,
        "M": bwd_low,
        "G": gradient,
        "N": bwd_grad0,
        "P": project_in,
        "PY": project_y,
        "PX": project_x,
        "PL": project_last,
        "PO": project_out,
        "S": z_sum,
        "SX": x_sum,
        "U": share_sum,
    }

    tiles_send()
    prepare(0, 0)
    third_blocks = block_loads(2, 0)
    for cp in third_blocks:
        cp.start()
    for k in range(NC):
        first_factor(k)
    prepare(1, 1)
    fourth_blocks = block_loads(3, 1)
    for cp in fourth_blocks:
        cp.start()
    pl.semaphore_wait(barrier, len(peers))
    pair_copy.start()
    for k in range(NC):
        fwd_out(1, k).start()

    for name, *args in ORDER:
        steps_of[name](*args)

    def sends_end():
        for m in (1, 2, 3):
            for way in range(2):
                for back in range(2):
                    wait_all_sent(way, m, back)
        for k in range(NC):
            p_last(k).wait_send()
        for k in (2, 3):
            p_core(k).wait_send()
            p_group(k).wait_send()
        pair_copy.wait_send()
        for m in range(4):
            z_three(m).wait_send()
            if m:
                u_send(m).wait_send()
            result(m).wait()
        x_four().wait_send()
        for k in range(NC):
            kv_result(k).wait()

    sends_end()


def finish(g, kv, mo, se, bl, ko, vo, nb, nm, ns, GV, KB, A, isem, jsem, osem):
    tok = lax.axis_index("tok")
    share = pl.ds(pl.multiple_of(tok * 32, 32), 32)
    copy = pltpu.make_async_copy

    def loads(m):
        return [
            copy(g.at[m], GV.at[m], isem.at[0, m]),
            copy(mo.at[m], A.at[0, m], isem.at[1, m]),
            copy(se.at[m], A.at[1, m], isem.at[2, m]),
            copy(bl.at[m, :, share, :], A.at[2, m], isem.at[3, m]),
        ]

    def stores(m):
        return [copy(A.at[i, m], out.at[m], osem.at[i, m]) for i, out in enumerate((nm, ns, nb))]

    kv_load = copy(kv, KB, jsem.at[0])
    kv_load.start()
    every = [loads(m) for m in range(4)]
    for group in every:
        for cp in group:
            cp.start()
    kv_load.wait()
    kv_stores = [
        copy(KB.at[pl.ds(0, 64)], ko, jsem.at[1]),
        copy(KB.at[pl.ds(64, 64)], vo, jsem.at[2]),
    ]
    for cp in kv_stores:
        cp.start()
    for m in range(4):
        for cp in every[m]:
            cp.wait()
        for c in range(4):
            for j in range(2):
                at = slice(j * 128, (j + 1) * 128)
                grad = GV[m, c, j]
                moment = beta_one * A[0, m, c, :, at] + (1.0 - beta_one) * grad
                second = beta_two * A[1, m, c, :, at] + (1.0 - beta_two) * grad * grad
                step = learn_rate * (moment / bias_one) / (jnp.sqrt(second / bias_two) + epsilon)
                A[0, m, c, :, at] = moment
                A[1, m, c, :, at] = second
                A[2, m, c, :, at] = A[2, m, c, :, at] - step
        for cp in stores(m):
            cp.start()
    for m in range(4):
        for cp in stores(m):
            cp.wait()
    for cp in kv_stores:
        cp.wait()


def local(x, kw, vw, bl, ro, kg, vg, mo, se):
    hbm = pl.BlockSpec(memory_space=pl.ANY)
    vmem = pl.BlockSpec(memory_space=pltpu.VMEM)
    dma = pltpu.SemaphoreType.DMA
    tile = (128, 128)
    scratch = [
        pltpu.VMEM((2, 2, 8) + tile, F32),
        pltpu.VMEM((2, 4, 1024, 256), BF16),
        pltpu.VMEM((2, 4, 1024, 256), BF16),
        pltpu.VMEM((4, 4, 256, 256), BF16),
        pltpu.VMEM((4, 4, 256, 256), BF16),
        pltpu.VMEM((4,) + tile, BF16),
        pltpu.VMEM((4,) + tile, BF16),
        pltpu.VMEM((4, 128, 1024), F32),
        pltpu.VMEM((8, 4) + tile, F32),
        pltpu.VMEM((4, 2, 4, 512, 128), F32),
        pltpu.VMEM((3, 4, 512, 128), F32),
        pltpu.VMEM((4, 4, 512, 128), F32),
        pltpu.VMEM((4, 2, 4, 512, 128), F32),
        pltpu.VMEM((3, 4, 512, 128), F32),
        pltpu.VMEM((2, 8, 512, 128), F32),
        pltpu.VMEM((512, 128), F32),
        pltpu.VMEM((512, 128), F32),
        pltpu.VMEM((2, 256, 1024), BF16),
        pltpu.VMEM((2, 256, 1024), BF16),
        pltpu.VMEM((3, 2) + tile, F32),
        pltpu.VMEM((2, 4) + tile, F32),
        pltpu.VMEM((7, 2) + tile, F32),
        pltpu.VMEM((4,) + tile, F32),
        pltpu.VMEM((4, 4, 2, 4, 2, 32, 128), F32),
        pltpu.VMEM((4, 3, 2, 4, 2, 32, 128), F32),
        pltpu.VMEM((4, 4, 2, 32, 128), F32),
        pltpu.VMEM((128, 512), F32),
        dma((4,)),
        dma((4, 8)),
        dma((4,)),
        dma((4,)),
        dma((2,)),
        dma((8,)),
        dma((2, 3, 2)),
        dma((2, 3, 2, 4)),
        dma((5,)),
        dma((5,)),
        dma((2, 2)),
        dma((2, 2)),
        dma((14,)),
        dma((14,)),
        dma((5,)),
        dma((5,)),
        dma((4,)),
        dma((4,)),
    ]
    share = jax.ShapeDtypeStruct((4, 4, 32, 256), F32)
    narrow = jax.ShapeDtypeStruct((64, 512), F32)
    grads, kv = pl.pallas_call(
        kernel,
        out_shape=(
            jax.ShapeDtypeStruct((4, 4, 2, 32, 128), F32),
            jax.ShapeDtypeStruct((128, 512), F32),
        ),
        in_specs=[hbm, hbm, hbm, hbm, vmem, hbm, hbm],
        out_specs=(hbm, hbm),
        scratch_shapes=scratch,
        compiler_params=pltpu.CompilerParams(
            collective_id=0, has_side_effects=True, vmem_limit_bytes=67043328
        ),
    )(x, kw, vw, bl, ro, kg.T, vg.T)
    ko, vo, nb, nm, ns = pl.pallas_call(
        finish,
        out_shape=(narrow, narrow, share, share, share),
        in_specs=[hbm] * 5,
        out_specs=(hbm,) * 5,
        scratch_shapes=[
            pltpu.VMEM((4, 4, 2, 32, 128), F32),
            pltpu.VMEM((128, 512), F32),
            pltpu.VMEM((3, 4, 4, 32, 256), F32),
            dma((4, 4)),
            dma((3,)),
            dma((3, 4)),
        ],
    )(grads, kv, mo, se, bl)
    return ko.T, vo.T, nb, nm, ns


def solution(mesh):
    placed = (
        P("tok", "feat"),
        P("feat", None),
        P("feat", None),
        P(None, "feat", None, None),
        P(),
        P("tok", "feat"),
        P("tok", "feat"),
        P(None, "feat", "tok", None),
        P(None, "feat", "tok", None),
    )
    return jax.shard_map(
        local,
        mesh=mesh,
        in_specs=placed,
        out_specs=(
            P("tok", "feat"),
            P("tok", "feat"),
            P(None, "feat", "tok", None),
            P(None, "feat", "tok", None),
            P(None, "feat", "tok", None),
        ),
        check_vma=False,
    )
```
